32 devices in a mesh: dp: 1 (over z), sp: 32 (over x, y, core).
Axes of the slice: x: 4, y: 4, z: 1, core: 2. Of those that a mesh axis runs over, the one named last changes fastest.
The devices are a block of a 4x4x8 slice.
Arguments:
- x: bfloat16 [4096, 4096], P(('dp', 'sp'))
- gain: bfloat16 [4096], replicated
- wq: bfloat16 [4096, 4096], replicated
- wk: bfloat16 [4096, 512], replicated
- wv: bfloat16 [4096, 512], replicated
- wo: bfloat16 [4096, 4096], replicated
Outputs:
- output: bfloat16 [4096, 4096], P(('dp', 'sp'))
All inputs are finite; a program needn't handle non-finite values.
Results may differ from the reference program's by a relative error of at most 0.012.
Values are sent between devices in bfloat16 or wider.
A program may use at most 768 MiB of HBM per device.

```python
import jax
import jax.numpy as jnp
from jax import lax

ROWS = 4096
D = 4096
HEADS = 32
KV_HEADS = 4
HEAD = 128
THETA = 10000


def setup_inputs(seed: int = 0, part: int = 0) -> dict:
    kx, kn, kq, kk, kv, ko = jax.random.split(jax.random.key(seed), 6)

    def weights(key, rows, columns):
        return jax.random.normal(key, (rows, columns), jnp.float32) * rows**-0.5

    drawn = {
        "x": jax.random.normal(jax.random.fold_in(kx, part), (ROWS, D), jnp.float32),
        "gain": 1 + 0.1 * jax.random.normal(kn, (D,), jnp.float32),
        "wq": 2 * weights(kq, D, HEADS * HEAD),
        "wk": 2 * weights(kk, D, KV_HEADS * HEAD),
        "wv": 4 * weights(kv, D, KV_HEADS * HEAD),
        "wo": weights(ko, HEADS * HEAD, D),
    }
    return {k: v.astype(jnp.bfloat16) for k, v in drawn.items()}


def normed(x, gain):
    wide = x.astype(jnp.float32)
    scale = lax.rsqrt(jnp.mean(wide * wide, -1, keepdims=True) + 1e-6)
    return (wide * scale * gain.astype(jnp.float32)).astype(jnp.bfloat16)


def turned(t, place, theta):
    half = t.shape[-1] // 2
    angle = place.astype(jnp.float32)[:, None] * theta ** (-jnp.arange(half, dtype=jnp.float32) / half)
    cos, sin = jnp.cos(angle)[:, None], jnp.sin(angle)[:, None]
    a, b = t[..., :half].astype(jnp.float32), t[..., half:].astype(jnp.float32)
    return jnp.concatenate([a * cos - b * sin, b * cos + a * sin], -1).astype(jnp.bfloat16)


def matmul(a, w):
    return jnp.dot(a, w, preferred_element_type=jnp.float32).astype(jnp.bfloat16)


def einsum(form, a, b):
    return jnp.einsum(form, a.astype(jnp.float32), b.astype(jnp.float32))


def attention(q, k, v):
    scores = einsum("tgsd,ugd->gstu", q, k) * q.shape[-1] ** -0.5
    token = jnp.arange(q.shape[0])
    scores = jnp.where(token[:, None] >= token, scores, -jnp.inf)
    weights = jax.nn.softmax(scores, -1).astype(jnp.bfloat16)
    return einsum("gstu,ugd->tgsd", weights, v).astype(jnp.bfloat16)


def reference(x, gain, wq, wk, wv, wo):
    a, place = normed(x, gain), jnp.arange(ROWS)
    q = turned(matmul(a, wq).reshape(ROWS, HEADS, HEAD), place, THETA).reshape(ROWS, KV_HEADS, -1, HEAD)
    k = turned(matmul(a, wk).reshape(ROWS, KV_HEADS, HEAD), place, THETA)
    v = matmul(a, wv).reshape(ROWS, KV_HEADS, HEAD)
    seen = attention(q, k, v).reshape(ROWS, HEADS * HEAD)
    return (x.astype(jnp.float32) + jnp.dot(seen, wo, preferred_element_type=jnp.float32)).astype(jnp.bfloat16)
```

```python
import functools
import math

import jax
import jax.numpy as jnp
import numpy as np
from jax import lax
from jax.experimental import pallas as pl
from jax.experimental.pallas import tpu as pltpu
from jax.sharding import PartitionSpec as P

HEAD = 128
THETA = 10000
HIDDEN = -2e30
NONE = -1e30
BIG = 1e30
LOG2E = 1.4426950408889634
VMEM = 67_043_328
MESH = pl.DeviceIdType.MESH
F32, BF16 = jnp.float32, jnp.bfloat16


def _dot(a, b, ca, cb):
    return lax.dot_general(a, b, (((ca,), (cb,)), ((), ())), preferred_element_type=F32)


GROUPS = (
    ((1, 0), (3, 0), (0, 1), (0, 3)),
    ((3, 3), (1, 1), (1, 3), (3, 1)),
    ((2, 0), (0, 2), (2, 1), (2, 3)),
    ((3, 2), (1, 2), (2, 2), None),
)


def _kernel(cfg, x_h, g_h, wq_h, wk_h, wv_h, wo_h, ta_h, tb_h, o_h,
            pool, xs, gs, a_s, xr, ta, tb, cs, stage_k, stage_v, kb, vb, q_s, mix_s, top_s, seen, accy, ybuf,
            wsem, lsem, ksem, vsem, ownsem, asem, xrsem, ssem, ysem, send):
    S, own, D, CW, NH = cfg
    T = 2 * own
    KV = 2
    NC = NH * HEAD // CW
    HC = CW // HEAD
    W = 2 * T
    NS = NH // 2
    e = HEAD**-0.5 * LOG2E

    me = lax.axis_index("sp")
    c = lax.rem(me, 2)
    chip = lax.div(me, 2)
    X, Y = lax.div(chip, S), lax.rem(chip, S)
    oc = 1 - c
    sg = 1 - 2 * c
    sib = chip * 2 + oc

    def at(a, b):
        return lax.rem(X + sg * a + S, S), lax.rem(Y + sg * b + S, S)

    def dev(xy, k):
        return (xy[0] * S + xy[1]) * 2 + k

    NX, PX, NY, PY = at(1, 0), at(-1, 0), at(0, 1), at(0, -1)

    def local(src, dst, sem):
        cp = pltpu.make_async_copy(src, dst, sem)
        cp.start()
        return cp

    x_cp = local(x_h, xs, lsem.at[0])
    g_cp = local(g_h, gs, lsem.at[1])
    wk_cp = local(wk_h, pool.at[0], wsem.at[0])
    wv_cp = local(wv_h, pool.at[1], wsem.at[1])
    ta_cp = local(ta_h, ta, lsem.at[2])
    tb_cp = local(tb_h, tb, lsem.at[3])

    barrier = pltpu.get_barrier_semaphore()
    greet = [sib] + [dev(n, k) for n in (NX, PX, NY, PY) for k in range(2)]
    for d in greet:
        pl.semaphore_signal(barrier, inc=1, device_id={"sp": d}, device_id_type=MESH)

    sent = []

    def push(src, dst, rsem, device):
        cp = pltpu.make_async_remote_copy(src_ref=src, dst_ref=dst, send_sem=send.at[len(sent)], recv_sem=rsem,
                                          device_id={"sp": device}, device_id_type=MESH)
        cp.start()
        sent.append((src, len(sent)))
        return cp

    def wait_for(ref, sem):
        pltpu.make_async_copy(ref, ref, sem).wait()

    def cols(k, j):
        return pl.ds(pl.multiple_of(k * (NH * HEAD) + j * CW, CW), CW)

    mine = pl.ds(pl.multiple_of(c * own, own), own)
    theirs = pl.ds(pl.multiple_of(oc * own, own), own)

    x_cp.wait()
    g_cp.wait()
    RG = 16

    def norm(r, _):
        rows = pl.ds(pl.multiple_of(r * RG, RG), RG)
        wide = xs[rows, :].astype(F32)
        scale = lax.rsqrt(jnp.sum(wide * wide, axis=-1, keepdims=True) * (1 / D) + 1e-6)
        a_s[pl.ds(pl.multiple_of(c * own + r * RG, RG), RG), :] = (wide * scale * gs[...].astype(F32)).astype(BF16)
        return 0

    lax.fori_loop(0, own // RG, norm, 0)
    pl.semaphore_wait(barrier, len(greet))
    push(a_s.at[mine, :], a_s.at[mine, :], asem, sib)

    ta_cp.wait()
    tb_cp.wait()
    cb, sb = tb[chip, 0:1, :], tb[chip, 1:2, :]
    ca, sa = ta[0], ta[1]
    cs[0] = ca * cb - sa * sb
    cs[1] = sa * cb + ca * sb

    def turned(t, cos, sin):
        t = t.astype(BF16).astype(F32)
        return (t * cos + pltpu.roll(t, HEAD // 2, 1) * sin).astype(BF16)

    def block(ref, xy, kind):
        span = pl.ds(pl.multiple_of(xy[1] * T, T), T)
        return ref.at[xy[0], :, span, :] if kind == 0 else ref.at[xy[0], :, :, span]

    def part(ref, xy, kind, k):
        span = pl.ds(pl.multiple_of(xy[1] * T + k * own, own), own)
        return ref.at[xy[0], :, span, :] if kind == 0 else ref.at[xy[0], :, :, span]

    me_xy = (X, Y)
    sems = (ksem, vsem)
    bufs = (kb, vb)
    stages = (stage_k, stage_v)

    def own_out(kind, n):
        for k in range(2):
            push(stages[kind].at[pl.ds(KV * k, KV)], part(bufs[kind], me_xy, kind, c), sems[kind].at[X, Y], dev(n, k))

    wk_cp.wait()
    k_all = _dot(a_s[mine, :], pool[0], 1, 0)
    cos, sin = cs[0, mine, :], cs[1, mine, :]
    for h in range(2 * KV):
        stage_k[h] = turned(k_all[:, h * HEAD : (h + 1) * HEAD], cos, sin)
    span = pl.ds(pl.multiple_of(Y * T + c * own, own), own)
    for h in range(KV):
        kb[X, h, span, :] = stage_k[KV * c + h]
    own_out(0, NX)
    own_out(0, PX)
    push(stage_k.at[pl.ds(KV * oc, KV)], part(kb, me_xy, 0, c), ownsem.at[0], sib)

    wv_cp.wait()
    v_all = _dot(a_s[mine, :], pool[1], 1, 0).astype(BF16)
    for h in range(2 * KV):
        stage_v[h] = v_all[:, h * HEAD : (h + 1) * HEAD].T
    for h in range(KV):
        vb[X, h, :, span] = stage_v[KV * c + h]
    own_out(1, NY)
    own_out(1, PY)
    own_out(0, NY)
    own_out(0, PY)
    own_out(1, NX)
    own_out(1, PX)
    push(stage_v.at[pl.ds(KV * oc, KV)], part(vb, me_xy, 1, c), ownsem.at[1], sib)

    wq_cp = [local(wq_h.at[:, cols(c, j)], pool.at[2 + j], wsem.at[2 + j]) for j in range(NC)]
    xr_cp = [local(x_h.at[:, cols(c, j)], xr.at[j, mine, :], lsem.at[4 + j]) for j in range(NC)]
    for j in range(NC):
        push(x_h.at[:, cols(oc, j)], xr.at[j, mine, :], xrsem.at[j], sib)

    def forward(kind, a, b):
        ax = (a, b) if kind == 0 else (b, a)
        xy = at(*ax)
        ref = block(bufs[kind], xy, kind)
        wait_for(ref, sems[kind].at[xy[0], xy[1]])
        one, two = ((NX, PX), (NY, PY)) if kind == 0 else ((NY, PY), (NX, PX))
        to = []
        if b == 0:
            if a == 3:
                to.append(one[0])
            to += [two[0], two[1]]
        elif b == 3:
            to.append(two[0])
        for n in to:
            push(ref, ref, sems[kind].at[xy[0], xy[1]], dev(n, c))

    def arrive(kind, a, b):
        xy = at(*((a, b) if kind == 0 else (b, a)))
        wait_for(block(bufs[kind], xy, kind), sems[kind].at[xy[0], xy[1]])

    wait_for(a_s.at[theirs, :], asem)
    wo_cp = [None] * NC

    def queries(j):
        wq_cp[j].wait()
        q = _dot(a_s[...], pool[2 + j], 1, 0)
        for i in range(HC):
            q_s[pl.ds((j * HC + i) * T, T), :] = turned(q[:, i * HEAD : (i + 1) * HEAD], cs[0], cs[1])

    def load_wo(j):
        wo_cp[j] = local(wo_h.at[:, cols(c, j)], pool.at[j], wsem.at[2 + NC + j])

    queries(0)
    load_wo(0)
    queries(1)
    load_wo(1)
    queries(2)
    forward(0, 3, 0)
    forward(0, 1, 0)
    load_wo(2)
    queries(3)
    forward(1, 3, 0)
    forward(1, 1, 0)
    load_wo(3)

    wait_for(part(kb, me_xy, 0, oc), ownsem.at[0])
    wait_for(part(vb, me_xy, 1, oc), ownsem.at[1])
    span = pl.ds(pl.multiple_of(Y * T, T), T)
    ok = lax.broadcasted_iota(jnp.int32, (T, W), 0) <= lax.rem(lax.broadcasted_iota(jnp.int32, (T, W), 1), T)

    def first(s, _):
        h = lax.div(s * KV, NS)
        q = q_s[pl.ds(pl.multiple_of(s * W, W), W), :]
        t = jnp.where(ok, _dot(kb[X, h, span, :], q, 1, 1), HIDDEN)
        top = t.max(axis=0, keepdims=True)
        p = jnp.exp2((t - top) * e).astype(BF16)
        v = jnp.concatenate([vb[X, h, :, span], jnp.ones((8, T), BF16)], axis=0)
        top_s[s] = top
        mix_s[s] = _dot(v, p, 1, 0)
        return 0

    lax.fori_loop(0, NS, first, 0)
    forward(1, 0, 3)
    forward(0, 0, 3)

    def strips(g, todo):
        spots = [at(*(b or (0, 0))) for b in GROUPS[g]]
        seen_j = [(xy[0] * S + xy[1] < chip) if b else None for xy, b in zip(spots, GROUPS[g])]
        spots = [xy for xy, s in zip(spots, seen_j) if s is not None]
        seen_j = [s for s in seen_j if s is not None]
        n = len(spots)
        spans = [pl.ds(pl.multiple_of(xy[1] * T, T), T) for xy in spots]
        any_seen = functools.reduce(jnp.logical_or, seen_j)

        def one(s):
            h = lax.div(s * KV, NS)
            q = q_s[pl.ds(pl.multiple_of(s * W, W), W), :]
            k = jnp.concatenate([kb[xy[0], h, sp, :] for xy, sp in zip(spots, spans)], axis=0)
            t = _dot(k, q, 1, 1)
            old = top_s[s]
            parts = [t[i * T : (i + 1) * T] for i in range(n)]
            tops = [jnp.where(seen_j[i], parts[i].max(axis=0, keepdims=True), NONE) for i in range(n)]
            top = functools.reduce(jnp.maximum, tops, old)
            top_s[s] = top
            p = jnp.concatenate(
                [jnp.exp2((parts[i] - jnp.where(seen_j[i], top, BIG)) * e).astype(BF16) for i in range(n)], axis=0)
            keep = jnp.exp2((old - top) * e)
            v = jnp.concatenate([vb[xy[0], h, :, sp] for xy, sp in zip(spots, spans)], axis=1)
            v = jnp.concatenate([v, jnp.ones((8, n * T), BF16)], axis=0)
            mix_s[s] = mix_s[s] * keep + _dot(v, p, 1, 0)

        def pair(i):
            @pl.when(any_seen)
            def _():
                one(2 * i)
                one(2 * i + 1)

        at_i = 0
        for upto, acts in todo:
            lax.fori_loop(at_i, upto, lambda i, _: (pair(i), 0)[1], 0)
            at_i = upto
            for f in acts:
                f()

    NP = NS // 2
    fw = lambda *a: functools.partial(forward, *a)
    arrive(0, 0, 1)
    arrive(1, 0, 1)
    strips(0, ((NP // 2, (fw(0, 2, 0),)), (NP - 1, (fw(0, 3, 3),)), (NP, ())))
    forward(1, 3, 3)
    forward(0, 1, 3)
    forward(1, 1, 3)
    for kind in range(2):
        arrive(kind, 1, 1)
        arrive(kind, 3, 1)
    strips(1, ((NP // 2, (fw(1, 2, 0),)), (NP, ())))
    forward(0, 2, 3)
    arrive(0, 2, 1)
    arrive(0, 0, 2)
    arrive(1, 0, 2)
    arrive(1, 1, 2)
    arrive(1, 3, 2)
    strips(2, ((NP // 2, (fw(1, 2, 3),)), (NP, ())))
    arrive(0, 3, 2)
    arrive(0, 1, 2)
    arrive(0, 2, 2)
    arrive(1, 2, 1)
    arrive(1, 2, 2)
    strips(3, ((NP, ()),))

    for s in range(NS):
        o = mix_s[s, :HEAD, :] * (1 / mix_s[s, HEAD : HEAD + 1, :])
        for i in range(2):
            seen[c, 2 * s + i] = o[:, i * T : (i + 1) * T].T.astype(BF16)
        two = seen.at[c, pl.ds(2 * s, 2)]
        push(two, two, ssem.at[s], sib)

    for j in range(NC):
        wo_cp[j].wait()

    def lhs(k):
        return jnp.concatenate([seen[k, i] for i in range(NH)], axis=1)

    def out_own(j, _):
        accy[j] = _dot(lhs(c), pool[j, pl.ds(pl.multiple_of(c * NH * HEAD, NH * HEAD), NH * HEAD), :], 1, 0)
        return 0

    lax.fori_loop(0, NC, out_own, 0)
    for s in range(NS):
        two = seen.at[oc, pl.ds(2 * s, 2)]
        wait_for(two, ssem.at[s])
    for j in range(NC):
        xr_cp[j].wait()
        wait_for(xr.at[j, theirs, :], xrsem.at[j])
    outs = []
    for j in range(NC):
        y = accy[j] + _dot(lhs(oc), pool[j, pl.ds(pl.multiple_of(oc * NH * HEAD, NH * HEAD), NH * HEAD), :], 1, 0)
        ybuf[j] = (xr[j].astype(F32) + y).astype(BF16)
        outs.append(local(ybuf.at[j, mine, :], o_h.at[:, cols(c, j)], lsem.at[4 + NC + j]))
        push(ybuf.at[j, theirs, :], o_h.at[:, cols(c, j)], ysem.at[j], sib)
    for j in range(NC):
        outs[j].wait()
        wait_for(o_h.at[:, cols(oc, j)], ysem.at[j])
    for ref, i in sent:
        wait_for(ref, send.at[i])


def solution(mesh):
    n = mesh.shape["sp"]
    chips = n // 2
    S = math.isqrt(chips)

    def tables(own):
        half = HEAD // 2
        rate = (np.float32(THETA) ** (-np.arange(half, dtype=np.float32) / np.float32(half))).astype(np.float64)

        def pair(place):
            angle = place[:, None] * rate
            cos, sin = np.cos(angle), np.sin(angle)
            return np.concatenate([cos, cos], 1), np.concatenate([-sin, sin], 1)

        ta = np.stack(pair(np.arange(2 * own, dtype=np.float64)))
        tb = np.stack(pair(np.arange(chips, dtype=np.float64) * 2 * own), 1)
        return ta.astype(np.float32), tb.astype(np.float32)

    def step(x, gain, wq, wk, wv, wo):
        own, D = x.shape
        NH = wq.shape[1] // HEAD // 2
        KV = wk.shape[1] // HEAD // 2
        CW = wk.shape[1]
        NC = NH * HEAD // CW
        T, W, NS = 2 * own, 4 * own, NH // 2
        ta, tb = tables(own)
        any_ = pl.BlockSpec(memory_space=pl.ANY)
        dma = pltpu.SemaphoreType.DMA
        return pl.pallas_call(
            functools.partial(_kernel, (S, own, D, CW, NH)),
            out_shape=jax.ShapeDtypeStruct(x.shape, x.dtype),
            in_specs=[any_] * 8,
            out_specs=any_,
            scratch_shapes=[
                pltpu.VMEM((2 + NC, D, CW), BF16),
                pltpu.VMEM((own, D), BF16),
                pltpu.VMEM((1, D), BF16),
                pltpu.VMEM((T, D), BF16),
                pltpu.VMEM((NC, T, CW), BF16),
                pltpu.VMEM((2, T, HEAD), F32),
                pltpu.VMEM((chips, 2, HEAD), F32),
                pltpu.VMEM((2, T, HEAD), F32),
                pltpu.VMEM((2 * KV, own, HEAD), BF16),
                pltpu.VMEM((2 * KV, HEAD, own), BF16),
                pltpu.VMEM((S, KV, S * T, HEAD), BF16),
                pltpu.VMEM((S, KV, HEAD, S * T), BF16),
                pltpu.VMEM((NH * T, HEAD), BF16),
                pltpu.VMEM((NS, HEAD + 8, W), F32),
                pltpu.VMEM((NS, 1, W), F32),
                pltpu.VMEM((2, NH, T, HEAD), BF16),
                pltpu.VMEM((NC, T, CW), F32),
                pltpu.VMEM((NC, T, CW), BF16),
                dma((2 + 2 * NC,)),
                dma((4 + 2 * NC,)),
                dma((S, S)),
                dma((S, S)),
                dma((2,)),
                dma,
                dma((NC,)),
                dma((NS,)),
                dma((NC,)),
                dma((80,)),
            ],
            compiler_params=pltpu.CompilerParams(collective_id=0, has_side_effects=True, vmem_limit_bytes=VMEM),
        )(x, gain[None], wq, wk, wv, wo, ta, tb)

    tokens, whole = P(("dp", "sp"), None), P(None, None)
    return jax.shard_map(
        step,
        mesh=mesh,
        in_specs=(tokens, P(None), whole, whole, whole, whole),
        out_specs=tokens,
        check_vma=False,
    )
```

```python
import functools
import math

import jax
import jax.numpy as jnp
import numpy as np
from jax import lax
from jax.experimental import pallas as pl
from jax.experimental.pallas import tpu as pltpu
from jax.sharding import PartitionSpec as P

HEAD = 128
THETA = 10000
HIDDEN = -2e30
NONE = -1e30
BIG = 1e30
LOG2E = 1.4426950408889634
VMEM = 60 * 2**20
MESH = pl.DeviceIdType.MESH
F32, BF16 = jnp.float32, jnp.bfloat16


def _dot(a, b, ca, cb):
    return lax.dot_general(a, b, (((ca,), (cb,)), ((), ())), preferred_element_type=F32)


GROUPS = (
    ((0, 0), (1, 0), (3, 0), (0, 1)),
    ((0, 3), (3, 3), (1, 1), (1, 3)),
    ((3, 1), (2, 0), (0, 2), (2, 1)),
    ((2, 3), (3, 2), (1, 2), (2, 2)),
)


def _kernel(cfg, x_h, g_h, wq_h, wk_h, wv_h, wo_h, ta_h, tb_h, o_h,
            pool, xs, gs, a_s, xr, ta, tb, cs, stage_k, stage_v, kb, vb, q_s, mix_s, top_s, seen, accy, ybuf,
            gap,
            wsem, lsem, ksem, vsem, ownsem, asem, xrsem, ssem, ysem, sends, send):
    S, own, D, CW, NH = cfg
    T = 2 * own
    KV = 2
    NC = NH * HEAD // CW
    HC = CW // HEAD
    W = 2 * T
    NS = NH // 2
    e = HEAD**-0.5 * LOG2E

    me = lax.axis_index("sp")
    c = lax.rem(me, 2)
    chip = lax.div(me, 2)
    X, Y = lax.div(chip, S), lax.rem(chip, S)
    oc = 1 - c
    sg = 1 - 2 * c
    sib = chip * 2 + oc

    @functools.cache
    def at(a, b):
        return lax.rem(X + sg * a + S, S), lax.rem(Y + sg * b + S, S)

    def dev(xy, k):
        return (xy[0] * S + xy[1]) * 2 + k

    for a_ in range(4):
        for b_ in range(4):
            at(a_, b_)
    NX, PX, NY, PY = at(1, 0), at(3, 0), at(0, 1), at(0, 3)

    def local(src, dst, sem):
        cp = pltpu.make_async_copy(src, dst, sem)
        cp.start()
        return cp

    x_cp = local(x_h, xs, lsem.at[0])
    g_cp = local(g_h, gs, lsem.at[1])
    wk_cp = local(wk_h, pool.at[0], wsem.at[0])
    wv_cp = local(wv_h, pool.at[1], wsem.at[1])
    ta_cp = local(ta_h, ta, lsem.at[2])
    tb_cp = local(tb_h, tb, lsem.at[3])

    barrier = pltpu.get_barrier_semaphore()
    greet = [sib] + [dev(n, k) for n in (NX, PX, NY, PY) for k in range(2)]
    for d in greet:
        pl.semaphore_signal(barrier, inc=1, device_id={"sp": d}, device_id_type=MESH)

    sent = []

    def push(src, dst, rsem, device, like=None):
        cp = pltpu.make_async_remote_copy(src_ref=src, dst_ref=dst, send_sem=send.at[len(sent)], recv_sem=rsem,
                                          device_id={"sp": device}, device_id_type=MESH)
        cp.start()
        sent.append((src if like is None else like, len(sent)))
        return cp

    def wait_for(ref, sem):
        pltpu.make_async_copy(ref, ref, sem).wait()

    def cols(k, j):
        return pl.ds(pl.multiple_of(k * (NH * HEAD) + j * CW, CW), CW)

    mine = pl.ds(pl.multiple_of(c * own, own), own)
    theirs = pl.ds(pl.multiple_of(oc * own, own), own)

    x_cp.wait()
    g_cp.wait()
    RG = 16

    def norm(r, _):
        rows = pl.ds(pl.multiple_of(r * RG, RG), RG)
        wide = xs[rows, :].astype(F32)
        scale = lax.rsqrt(jnp.sum(wide * wide, axis=-1, keepdims=True) * (1 / D) + 1e-6)
        a_s[pl.ds(pl.multiple_of(c * own + r * RG, RG), RG), :] = (wide * scale * gs[...].reshape(1, D).astype(F32)).astype(BF16)
        return 0

    lax.fori_loop(0, own // RG, norm, 0)
    pl.semaphore_wait(barrier, len(greet))
    push(a_s.at[mine, :], a_s.at[mine, :], asem, sib)

    ta_cp.wait()
    tb_cp.wait()
    cb, sb = tb[chip, 0:1, :], tb[chip, 1:2, :]
    ca, sa = ta[0], ta[1]
    cs[0] = ca * cb - sa * sb
    cs[1] = sa * cb + ca * sb

    def turned(t, cos, sin):
        t = t.astype(BF16).astype(F32)
        return (t * cos + pltpu.roll(t, HEAD // 2, 1) * sin).astype(BF16)

    def block(ref, xy, kind):
        span = pl.ds(pl.multiple_of(xy[1] * T, T), T)
        return ref.at[xy[0], :, span, :] if kind == 0 else ref.at[xy[0], :, :, span]

    def part(ref, xy, kind, k):
        span = pl.ds(pl.multiple_of(xy[1] * T + k * own, own), own)
        return ref.at[xy[0], :, span, :] if kind == 0 else ref.at[xy[0], :, :, span]

    me_xy = (X, Y)
    sems = (ksem, vsem)
    bufs = (kb, vb)
    stages = (stage_k, stage_v)
    whole = (block(kb, me_xy, 0), block(vb, me_xy, 1))

    def own_out(kind, n):
        for k in range(2):
            push(stages[kind].at[pl.ds(KV * k, KV)], part(bufs[kind], me_xy, kind, c), sems[kind].at[X, Y], dev(n, k))

    def load_wq(j):
        return pltpu.make_async_copy(wq_h.at[:, cols(c, j)], pool.at[2 + j], wsem.at[2 + j])

    def load_wo(j):
        return pltpu.make_async_copy(wo_h.at[:, cols(c, j)], pool.at[j], wsem.at[2 + NC + j])

    wk_cp.wait()
    for j in range(NC // 2):
        load_wq(j).start()
    k_all = _dot(a_s[mine, :], pool[0], 1, 0)
    cos, sin = cs[0, mine, :], cs[1, mine, :]
    for h in range(2 * KV):
        stage_k[h] = turned(k_all[:, h * HEAD : (h + 1) * HEAD], cos, sin)
    span = pl.ds(pl.multiple_of(Y * T + c * own, own), own)
    for h in range(KV):
        kb[X, h, span, :] = stage_k[KV * c + h]
    own_out(0, NX)
    own_out(0, PX)
    push(stage_k.at[pl.ds(KV * oc, KV)], part(kb, me_xy, 0, c), ownsem.at[0], sib)

    wv_cp.wait()
    for j in range(NC // 2, NC):
        load_wq(j).start()
    v_all = _dot(a_s[mine, :], pool[1], 1, 0).astype(BF16)
    for h in range(2 * KV):
        stage_v[h] = v_all[:, h * HEAD : (h + 1) * HEAD].T
    for h in range(KV):
        vb[X, h, :, span] = stage_v[KV * c + h]
    own_out(1, NY)
    own_out(1, PY)
    own_out(0, NY)
    own_out(0, PY)
    own_out(1, NX)
    own_out(1, PX)
    push(stage_v.at[pl.ds(KV * oc, KV)], part(vb, me_xy, 1, c), ownsem.at[1], sib)

    xr_cp = [local(x_h.at[:, cols(c, j)], xr.at[j, mine, :], lsem.at[4 + j]) for j in range(NC)]
    for j in range(NC):
        push(x_h.at[:, cols(oc, j)], xr.at[j, mine, :], xrsem.at[j], sib)

    def forward(kind, a, b):
        ax = (a, b) if kind == 0 else (b, a)
        xy = at(*ax)
        ref = block(bufs[kind], xy, kind)
        wait_for(ref, sems[kind].at[xy[0], xy[1]])
        one, two = ((NX, PX), (NY, PY)) if kind == 0 else ((NY, PY), (NX, PX))
        to = []
        if b == 0:
            if a == 3:
                to.append(one[0])
            to += [two[0], two[1]]
        elif b == 3:
            to.append(two[0])
        for n in to:
            push(ref, ref, sems[kind].at[xy[0], xy[1]], dev(n, c), like=whole[kind])

    def arrive(kind, a, b):
        xy = at(*((a, b) if kind == 0 else (b, a)))
        wait_for(block(bufs[kind], xy, kind), sems[kind].at[xy[0], xy[1]])

    wait_for(a_s.at[theirs, :], asem)

    def queries(j, _):
        load_wq(j).wait()
        q = _dot(a_s[...], pool[2 + j], 1, 0)
        for i in range(HC):
            rows = pl.ds(pl.multiple_of((j * HC + i) * T, T), T)
            q_s[rows, :] = turned(q[:, i * HEAD : (i + 1) * HEAD], cs[0], cs[1])
        load_wo(j).start()

        @pl.when(j == NC - 2)
        def _():
            forward(0, 3, 0)
            forward(0, 1, 0)

        return 0

    lax.fori_loop(0, NC, queries, 0)
    forward(1, 3, 0)
    forward(1, 1, 0)
    gap[...] = lax.rem(lax.broadcasted_iota(jnp.int32, (T, W), 1), T) - lax.broadcasted_iota(jnp.int32, (T, W), 0)
    top_s[...] = jnp.full(top_s.shape, NONE, F32)
    mix_s[...] = jnp.zeros(mix_s.shape, F32)

    wait_for(part(kb, me_xy, 0, oc), ownsem.at[0])
    wait_for(part(vb, me_xy, 1, oc), ownsem.at[1])
    arrive(1, 0, 1)
    forward(1, 0, 3)
    arrive(0, 0, 1)
    forward(0, 0, 3)

    U = 2
    per = NS // U
    acts = {
        0: ((0, 2, 0, 1),),
        1: ((0, 3, 3, 1),),
        2: ((1, 3, 3, 1),),
        3: ((0, 1, 3, 1), (1, 1, 3, 1), (0, 1, 1, 0), (1, 1, 1, 0), (1, 3, 1, 0)),
        4: ((1, 2, 0, 1),),
        6: ((0, 2, 3, 1),),
        7: ((1, 2, 3, 1), (0, 3, 1, 0), (1, 0, 2, 0), (0, 0, 2, 0), (0, 2, 1, 0), (1, 1, 2, 0)),
        11: ((1, 3, 2, 0), (0, 3, 2, 0), (0, 1, 2, 0), (1, 2, 1, 0), (0, 2, 2, 0), (1, 2, 2, 0)),
    }

    def pick(g, values):
        out = values[0]
        for n in range(1, len(values)):
            out = jnp.where(g == n, values[n], out)
        return out

    spots = [[at(*b) for b in g] for g in GROUPS]
    n = len(GROUPS[0])

    def step(t, _):
        g, i = lax.div(t, per), lax.rem(t, per)
        xs_ = [pick(g, [spots[m][j][0] for m in range(len(GROUPS))]) for j in range(n)]
        ys_ = [pick(g, [spots[m][j][1] for m in range(len(GROUPS))]) for j in range(n)]
        spans = [pl.ds(pl.multiple_of(y * T, T), T) for y in ys_]
        vis = [x * S + y <= chip for x, y in zip(xs_, ys_)]
        level = jnp.where(g == 0, 0, -T)

        def score(s):
            h = lax.div(s * KV, NS)
            q = q_s[pl.ds(pl.multiple_of(s * W, W), W), :]
            k = jnp.concatenate([kb[x, h, sp, :] for x, sp in zip(xs_, spans)], axis=0)
            return _dot(k, q, 1, 1)

        def rest(s, t):
            h = lax.div(s * KV, NS)
            old = top_s[s]
            parts = [t[m * T : (m + 1) * T] for m in range(n)]
            parts[0] = jnp.where(gap[...] >= level, parts[0], HIDDEN)
            tops = [jnp.where(vis[m], parts[m].max(axis=0, keepdims=True), NONE) for m in range(n)]
            top = functools.reduce(jnp.maximum, tops, old)
            top_s[s] = top
            p = jnp.concatenate(
                [jnp.exp2((parts[m] - jnp.where(vis[m], top, BIG)) * e).astype(BF16) for m in range(n)], axis=0)
            keep = jnp.exp2((old - top) * e)
            v = jnp.concatenate([vb[x, h, :, sp] for x, sp in zip(xs_, spans)], axis=1)
            v = jnp.concatenate([v, jnp.ones((8, n * T), BF16)], axis=0)
            mix_s[s] = mix_s[s] * keep + _dot(v, p, 1, 0)

        @pl.when(functools.reduce(jnp.logical_or, vis))
        def _():
            ts = [score(U * i + u) for u in range(U)]
            for u in range(U):
                rest(U * i + u, ts[u])

        for when, todo in acts.items():

            @pl.when(t == when)
            def _():
                for kind, a, b, on in todo:
                    (forward if on else arrive)(kind, a, b)

        return 0

    lax.fori_loop(0, per * len(GROUPS), step, 0)

    def share(s):
        two = seen.at[c, pl.ds(2 * s, 2)]
        return pltpu.make_async_remote_copy(src_ref=two, dst_ref=two, send_sem=sends.at[s], recv_sem=ssem.at[s],
                                            device_id={"sp": sib}, device_id_type=MESH)

    def finish(s, _):
        o = mix_s[s, :HEAD, :] * (1 / mix_s[s, HEAD : HEAD + 1, :])
        for i in range(2):
            seen[c, 2 * s + i] = o[:, i * T : (i + 1) * T].T.astype(BF16)
        share(s).start()
        return 0

    lax.fori_loop(0, NS, finish, 0)

    def lhs(k):
        return jnp.concatenate([seen[k, i] for i in range(NH)], axis=1)

    def share_of(k, j):
        return _dot(lhs(k), pool[j, pl.ds(pl.multiple_of(k * NH * HEAD, NH * HEAD), NH * HEAD), :], 1, 0)

    def out_own(j, _):
        load_wo(j).wait()
        accy[j] = share_of(c, j)
        return 0

    lax.fori_loop(0, NC, out_own, 0)
    for s in range(NS):
        share(s).wait()
    for j in range(NC):
        xr_cp[j].wait()
        wait_for(xr.at[j, theirs, :], xrsem.at[j])

    def out_there(j, k):
        return pltpu.make_async_remote_copy(src_ref=ybuf.at[j, theirs, :], dst_ref=o_h.at[:, cols(k, j)], send_sem=sends.at[NS + j],
                                            recv_sem=ysem.at[j], device_id={"sp": sib}, device_id_type=MESH)

    def out_rest(j, _):
        y = accy[j] + share_of(oc, j)
        ybuf[j] = (xr[j].astype(F32) + y).astype(BF16)
        out_there(j, c).start()
        o_h[:, cols(c, j)] = ybuf[j, mine, :]
        return 0

    lax.fori_loop(0, NC, out_rest, 0)
    for ref, i in sent:
        wait_for(ref, send.at[i])
    for j in range(NC):
        out_there(j, oc).wait()


def solution(mesh):
    n = mesh.shape["sp"]
    chips = n // 2
    S = math.isqrt(chips)

    def tables(own):
        half = HEAD // 2
        rate = (np.float32(THETA) ** (-np.arange(half, dtype=np.float32) / np.float32(half))).astype(np.float64)

        def pair(place):
            angle = place[:, None] * rate
            cos, sin = np.cos(angle), np.sin(angle)
            return np.concatenate([cos, cos], 1), np.concatenate([-sin, sin], 1)

        ta = np.stack(pair(np.arange(2 * own, dtype=np.float64)))
        tb = np.stack(pair(np.arange(chips, dtype=np.float64) * 2 * own), 1)
        return ta.astype(np.float32), tb.astype(np.float32)

    def step(x, gain, wq, wk, wv, wo):
        own, D = x.shape
        NH = wq.shape[1] // HEAD // 2
        KV = wk.shape[1] // HEAD // 2
        CW = wk.shape[1]
        NC = NH * HEAD // CW
        T, W, NS = 2 * own, 4 * own, NH // 2
        ta, tb = tables(own)
        any_ = pl.BlockSpec(memory_space=pl.ANY)
        dma = pltpu.SemaphoreType.DMA
        return pl.pallas_call(
            functools.partial(_kernel, (S, own, D, CW, NH)),
            out_shape=pltpu.VMEM(x.shape, x.dtype),
            in_specs=[any_] * 8,
            out_specs=pl.BlockSpec(memory_space=pltpu.VMEM),
            scratch_shapes=[
                pltpu.VMEM((2 + NC, D, CW), BF16),
                pltpu.VMEM((own, D), BF16),
                pltpu.VMEM((D,), BF16),
                pltpu.VMEM((T, D), BF16),
                pltpu.VMEM((NC, T, CW), BF16),
                pltpu.VMEM((2, T, HEAD), F32),
                pltpu.VMEM((chips, 2, HEAD), F32),
                pltpu.VMEM((2, T, HEAD), F32),
                pltpu.VMEM((2 * KV, own, HEAD), BF16),
                pltpu.VMEM((2 * KV, HEAD, own), BF16),
                pltpu.VMEM((S, KV, S * T, HEAD), BF16),
                pltpu.VMEM((S, KV, HEAD, S * T), BF16),
                pltpu.VMEM((NH * T, HEAD), BF16),
                pltpu.VMEM((NS, HEAD + 8, W), F32),
                pltpu.VMEM((NS, 1, W), F32),
                pltpu.VMEM((2, NH, T, HEAD), BF16),
                pltpu.VMEM((NC, T, CW), F32),
                pltpu.VMEM((NC, T, CW), BF16),
                pltpu.VMEM((T, W), jnp.int32),
                dma((2 + 2 * NC,)),
                dma((4 + 2 * NC,)),
                dma((S, S)),
                dma((S, S)),
                dma((2,)),
                dma,
                dma((NC,)),
                dma((NS,)),
                dma((NC,)),
                dma((NS + NC,)),
                dma((80,)),
            ],
            compiler_params=pltpu.CompilerParams(collective_id=0, has_side_effects=True, vmem_limit_bytes=VMEM),
        )(x, gain, wq, wk, wv, wo, ta, tb)

    tokens, whole = P(("dp", "sp"), None), P(None, None)
    return jax.shard_map(
        step,
        mesh=mesh,
        in_specs=(tokens, P(None), whole, whole, whole, whole),
        out_specs=tokens,
        check_vma=False,
    )
```

```python
import functools
import math

import jax
import jax.numpy as jnp
import numpy as np
from jax import lax
from jax.experimental import pallas as pl
from jax.experimental.pallas import tpu as pltpu
from jax.sharding import PartitionSpec as P

HEAD = 128
THETA = 10000
HIDDEN = -2e30
NONE = -1e30
BIG = 1e30
LOG2E = 1.4426950408889634
VMEM = 60 * 2**20
MESH = pl.DeviceIdType.MESH
F32, BF16 = jnp.float32, jnp.bfloat16


def _dot(a, b, ca, cb):
    return lax.dot_general(a, b, (((ca,), (cb,)), ((), ())), preferred_element_type=F32)


BLOCKS = ((0, 0), (1, 0), (3, 0), (0, 1), (0, 3), (3, 3), (1, 1), (1, 3), (3, 1), (2, 0), (0, 2), (2, 1), (2, 3), (3, 2), (1, 2), (2, 2))
EVENTS = (
    (1, 3, 0), (1, 1, 0), (0, 0, 3), (0, 0, 1), (0, 2, 0), (1, 1, 3), (0, 3, 3), (0, 3, 1), (1, 3, 3), (1, 1, 1), (0, 1, 3), (0, 1, 1), (1, 3, 1),
    (1, 2, 0), (1, 0, 2), (0, 2, 1), (1, 2, 3), (0, 0, 2), (1, 2, 1), (0, 2, 3), (0, 3, 2), (1, 1, 2), (1, 3, 2), (0, 1, 2), (0, 2, 2), (1, 2, 2),
)
TIMES = (140, 140, 147, 147, 167, 169, 175, 175, 196, 197, 203, 203, 210, 224, 231, 231, 239, 246, 254, 260, 274, 279, 281, 288, 302, 315)
START, STEP = 145, 16


def _kernel(cfg, x_h, g_h, wq_h, wk_h, wv_h, wo_h, ta_h, tb_h, o_h,
            pool, xs, gs, a_s, xr, ta, tb, cs, stage_k, stage_v, kb, vb, q_s, mix_s, top_s, seen, accy, ybuf,
            gap, sc0, sc1, mx0, mx1,
            wsem, lsem, ksem, vsem, ownsem, asem, xrsem, ssem, ysem, sends, send):
    sc, mx = (sc0, sc1), (mx0, mx1)
    S, own, D, CW, NH = cfg
    T = 2 * own
    KV = 2
    NC = NH * HEAD // CW
    HC = CW // HEAD
    W = 2 * T
    NS = NH // 2
    e = HEAD**-0.5 * LOG2E

    me = lax.axis_index("sp")
    c = lax.rem(me, 2)
    chip = lax.div(me, 2)
    X, Y = lax.div(chip, S), lax.rem(chip, S)
    oc = 1 - c
    sg = 1 - 2 * c
    sib = chip * 2 + oc

    @functools.cache
    def at(a, b):
        return lax.rem(X + sg * a + S, S), lax.rem(Y + sg * b + S, S)

    def dev(xy, k):
        return (xy[0] * S + xy[1]) * 2 + k

    for a_ in range(4):
        for b_ in range(4):
            at(a_, b_)
    NX, PX, NY, PY = at(1, 0), at(3, 0), at(0, 1), at(0, 3)

    def local(src, dst, sem):
        cp = pltpu.make_async_copy(src, dst, sem)
        cp.start()
        return cp

    x_cp = local(x_h, xs, lsem.at[0])
    g_cp = local(g_h, gs, lsem.at[1])
    wk_cp = local(wk_h, pool.at[0], wsem.at[0])
    wv_cp = local(wv_h, pool.at[1], wsem.at[1])
    ta_cp = local(ta_h, ta, lsem.at[2])
    tb_cp = local(tb_h, tb, lsem.at[3])

    barrier = pltpu.get_barrier_semaphore()
    greet = [sib] + [dev(n, k) for n in (NX, PX, NY, PY) for k in range(2)]
    for d in greet:
        pl.semaphore_signal(barrier, inc=1, device_id={"sp": d}, device_id_type=MESH)

    sent = []

    def needs(kind, s, d, sg=sg):
        (sx, sy), (dx, dy) = s, d
        ahead = lambda v: lax.rem(v + sg + S, S)
        if kind == 0:
            along = (sx < dx) | ((ahead(sx) == dx) & (sx < ahead(dx)))
            across = (sx < dx) | ((sx == dx) & ((sy < dy) | ((ahead(sy) == dy) & (sy < ahead(dy)))))
            return jnp.where(sy == dy, along, across)
        along = (sx < S - 1) | (sy < dy) | ((ahead(sy) == dy) & (sy < ahead(dy)))
        across = (sx < dx) | ((ahead(sx) == dx) & (sx < ahead(dx)))
        return jnp.where(sx == dx, along, across)

    def push(src, dst, rsem, device, like=None, cond=None):
        cp = pltpu.make_async_remote_copy(src_ref=src, dst_ref=dst, send_sem=send.at[len(sent)], recv_sem=rsem,
                                          device_id={"sp": device}, device_id_type=MESH)
        if cond is None:
            cp.start()
        else:
            pl.when(cond)(cp.start)
        sent.append((src if like is None else like, len(sent), cond))

    def wait_for(ref, sem):
        pltpu.make_async_copy(ref, ref, sem).wait()

    def cols(k, j):
        return pl.ds(pl.multiple_of(k * (NH * HEAD) + j * CW, CW), CW)

    mine = pl.ds(pl.multiple_of(c * own, own), own)
    theirs = pl.ds(pl.multiple_of(oc * own, own), own)

    def load_wq(j):
        return pltpu.make_async_copy(wq_h.at[:, cols(c, j)], pool.at[2 + j], wsem.at[2 + j])

    def load_wo(j):
        return pltpu.make_async_copy(wo_h.at[:, cols(c, j)], pool.at[j], wsem.at[2 + NC + j])

    x_cp.wait()
    g_cp.wait()
    RG = 16

    def norm(r, _):
        rows = pl.ds(pl.multiple_of(r * RG, RG), RG)
        wide = xs[rows, :].astype(F32)
        scale = lax.rsqrt(jnp.sum(wide * wide, axis=-1, keepdims=True) * (1 / D) + 1e-6)
        a_s[pl.ds(pl.multiple_of(c * own + r * RG, RG), RG), :] = (wide * scale * gs[...].reshape(1, D).astype(F32)).astype(BF16)
        return 0

    lax.fori_loop(0, own // RG, norm, 0)
    for j in range(NC // 2):
        load_wq(j).start()
    pl.semaphore_wait(barrier, len(greet))
    push(a_s.at[mine, :], a_s.at[mine, :], asem, sib)

    ta_cp.wait()
    tb_cp.wait()
    cb, sb = tb[chip, 0:1, :], tb[chip, 1:2, :]
    ca, sa = ta[0], ta[1]
    cs[0] = ca * cb - sa * sb
    cs[1] = sa * cb + ca * sb

    def turned(t, cos, sin):
        t = t.astype(BF16).astype(F32)
        return (t * cos + pltpu.roll(t, HEAD // 2, 1) * sin).astype(BF16)

    def block(ref, xy, kind):
        span = pl.ds(pl.multiple_of(xy[1] * T, T), T)
        return ref.at[xy[0], :, span, :] if kind == 0 else ref.at[xy[0], :, :, span]

    def part(ref, xy, kind, k):
        span = pl.ds(pl.multiple_of(xy[1] * T + k * own, own), own)
        return ref.at[xy[0], :, span, :] if kind == 0 else ref.at[xy[0], :, :, span]

    me_xy = (X, Y)
    sems = (ksem, vsem)
    bufs = (kb, vb)
    stages = (stage_k, stage_v)
    whole = (block(kb, me_xy, 0), block(vb, me_xy, 1))

    def own_out(kind, n):
        for k in range(2):
            push(stages[kind].at[pl.ds(KV * k, KV)], part(bufs[kind], me_xy, kind, c), sems[kind].at[X, Y], dev(n, k), cond=needs(kind, me_xy, n, 1 - 2 * k))

    wk_cp.wait()
    for j in range(NC // 2, NC):
        load_wq(j).start()
    k_all = _dot(a_s[mine, :], pool[0], 1, 0)
    cos, sin = cs[0, mine, :], cs[1, mine, :]
    for h in range(2 * KV):
        stage_k[h] = turned(k_all[:, h * HEAD : (h + 1) * HEAD], cos, sin)
    span = pl.ds(pl.multiple_of(Y * T + c * own, own), own)
    for h in range(KV):
        kb[X, h, span, :] = stage_k[KV * c + h]
    own_out(0, NX)
    own_out(0, PX)
    push(stage_k.at[pl.ds(KV * oc, KV)], part(kb, me_xy, 0, c), ownsem.at[0], sib)

    wv_cp.wait()
    v_all = _dot(a_s[mine, :], pool[1], 1, 0).astype(BF16)
    for h in range(2 * KV):
        stage_v[h] = v_all[:, h * HEAD : (h + 1) * HEAD].T
    for h in range(KV):
        vb[X, h, :, span] = stage_v[KV * c + h]
    own_out(1, NY)
    own_out(1, PY)
    own_out(0, NY)
    own_out(0, PY)
    own_out(1, NX)
    own_out(1, PX)
    push(stage_v.at[pl.ds(KV * oc, KV)], part(vb, me_xy, 1, c), ownsem.at[1], sib)

    xr_cp = [local(x_h.at[:, cols(c, j)], xr.at[j, mine, :], lsem.at[4 + j]) for j in range(NC)]
    for j in range(NC):
        push(x_h.at[:, cols(oc, j)], xr.at[j, mine, :], xrsem.at[j], sib)

    routes = {}
    for kind in range(2):
        one, two = ((NX, PX), (NY, PY)) if kind == 0 else ((NY, PY), (NX, PX))
        for a in range(4):
            for b in range(4):
                xy = at(*((a, b) if kind == 0 else (b, a)))
                to = ([one[0]] if a == 3 else []) + [two[0], two[1]] if b == 0 else [two[0]] if b == 3 else []
                if (a, b) != (0, 0):
                    routes[kind, a, b] = xy, needs(kind, xy, me_xy), [(n, needs(kind, xy, n)) for n in to]

    def forward(kind, a, b):
        xy, here, to = routes[kind, a, b]
        ref = block(bufs[kind], xy, kind)
        sem = sems[kind].at[xy[0], xy[1]]

        @pl.when(here)
        def _():
            wait_for(ref, sem)

        for n, cond in to:
            push(ref, ref, sem, dev(n, c), like=whole[kind], cond=cond)

    wait_for(a_s.at[theirs, :], asem)

    def queries(j, _):
        load_wq(j).wait()
        q = _dot(a_s[...], pool[2 + j], 1, 0)
        for i in range(HC):
            rows = pl.ds(pl.multiple_of((j * HC + i) * T, T), T)
            q_s[rows, :] = turned(q[:, i * HEAD : (i + 1) * HEAD], cs[0], cs[1])
        load_wo(j).start()

        @pl.when(j == NC - 2)
        def _():
            forward(0, 3, 0)
            forward(0, 1, 0)

        return 0

    lax.fori_loop(0, NC, queries, 0)
    forward(1, 3, 0)
    forward(1, 1, 0)
    gap[...] = lax.rem(lax.broadcasted_iota(jnp.int32, (T, W), 1), T) - lax.broadcasted_iota(jnp.int32, (T, W), 0)
    top_s[...] = jnp.full(top_s.shape, NONE, F32)
    mix_s[...] = jnp.zeros(mix_s.shape, F32)

    wait_for(part(kb, me_xy, 0, oc), ownsem.at[0])
    wait_for(part(vb, me_xy, 1, oc), ownsem.at[1])
    U = 2
    n = 4
    per = NS // U
    last = len(EVENTS) - 1
    rank, code = [], []
    nv = 0
    for a, b in BLOCKS:
        x, y = at(a, b)
        vis = x * S + y <= chip
        need = max([i for i, (_, p, q) in enumerate(EVENTS) if (p, q) == (a, b)], default=0)
        rank.append(jnp.where(vis, nv, -1))
        code.append((1 << 16) + (need << 8) + (x << 4) + y)
        nv = nv + vis.astype(jnp.int32)
        if len(rank) == n + 1:
            nv = jnp.maximum(nv, n)
    groups = jnp.where((lax.rem(nv, n) == n - 1) | (nv < n), lax.div(nv + n - 1, n), lax.div(nv, n))
    singles = jnp.maximum(nv - n * groups, 0)

    slots_ = []
    for k in range(len(BLOCKS)):
        got = functools.reduce(jnp.add, [jnp.where(r == k, v, 0) for r, v in zip(rank, code)])
        slots_.append(jnp.where(got > 0, got, code[0] - (1 << 16)))

    def pick(k, values):
        out = values[0]
        for i in range(1, len(values)):
            out = jnp.where(k == i, values[i], out)
        return out

    def score(s, slots):
        h = lax.div(s * KV, NS)
        q = q_s[pl.ds(pl.multiple_of(s * W, W), W), :]
        k = [kb[x, h, pl.ds(pl.multiple_of(y * T, T), T), :] for _, x, y, _ in slots]
        return _dot(jnp.concatenate(k, axis=0), q, 1, 1)

    def take(s, slots, parts, tops):
        h = lax.div(s * KV, NS)
        old = top_s[s]
        tops = [jnp.where(slot[3], top, NONE) for slot, top in zip(slots, tops)]
        top = functools.reduce(jnp.maximum, tops, old)
        top_s[s] = top
        p = [jnp.exp2((parts(i) - jnp.where(slot[3], top, BIG)) * e).astype(BF16) for i, slot in enumerate(slots)]
        keep = jnp.exp2((old - top) * e)
        v = [vb[x, h, :, pl.ds(pl.multiple_of(y * T, T), T)] for _, x, y, _ in slots]
        v = jnp.concatenate([jnp.concatenate(v, axis=1), jnp.ones((8, len(slots) * T), BF16)], axis=0)
        mix_s[s] = mix_s[s] * keep + _dot(v, jnp.concatenate(p, axis=0), 1, 0)

    def split(t, m):
        return [t[i * T : (i + 1) * T] for i in range(m)]

    def put(s, b, slots, cut):
        t = split(score(s, slots), n)
        if cut:
            t[0] = jnp.where(gap[...] >= 0, t[0], HIDDEN)
        for i in range(n):
            sc[b][i * T : (i + 1) * T, :] = t[i]
        mx[b][...] = jnp.concatenate([v.max(axis=0, keepdims=True) for v in t], axis=0)

    def fin(s, b, slots):
        take(s, slots, lambda i: sc[b][i * T : (i + 1) * T, :], [mx[b][i : i + 1, :] for i in range(n)])

    def pair(i, slots, cut):
        put(2 * i + 1, 1, slots, cut)
        fin(2 * i, 0, slots)
        put(jnp.minimum(2 * i + 2, NS - 1), 0, slots, cut)
        fin(2 * i + 1, 1, slots)

    def single(slots):
        ts = [score(s, slots) for s in range(NS)]
        for s, t in enumerate(ts):
            take(s, slots, lambda i: t, [t.max(axis=0, keepdims=True)])

    def step(t, carry):
        done, clock = carry
        g = lax.div(t, per)
        grouped = t < per * groups
        k = jnp.where(grouped, n * g, n * groups + t - per * groups)
        got = [pick(g, slots_[j::n]) for j in range(n)]
        got[0] = jnp.where(grouped, got[0], pick(k, slots_))
        slots = [((v >> 8) & 255, (v >> 4) & 15, v & 15, v >= 1 << 16) for v in got]
        target = functools.reduce(jnp.maximum, [jnp.where(slots[j][3] & (grouped | (j == 0)), slots[j][0], 0) for j in range(n)])
        for i, time in enumerate(TIMES):
            clock = jnp.maximum(clock, jnp.where(target == i, time, 0))
        come = functools.reduce(jnp.add, [jnp.where(clock >= time, 1, 0) for time in TIMES])
        target = jnp.maximum(target, come - 1)
        target = jnp.where(t == per * groups + singles, last, target)

        @pl.when(target > done)
        def _():
            for i, (kind, a, b) in enumerate(EVENTS):

                @pl.when((i > done) & (i <= target))
                def _():
                    forward(kind, *((a, b) if kind == 0 else (b, a)))

        i = lax.rem(t, per)

        for cut in (True, False):
            these = (g == 0) if cut else (grouped & (g > 0))

            @pl.when(these & (i == 0))
            def _():
                put(0, 0, slots, cut)

            @pl.when(these)
            def _():
                pair(i, slots, cut)

        @pl.when((t >= per * groups) & (t < per * groups + singles))
        def _():
            single(slots[:1])

        return jnp.maximum(done, target), clock + STEP

    lax.fori_loop(0, per * groups + singles + 1, step, (-1, START))

    def share(s):
        two = seen.at[c, pl.ds(2 * s, 2)]
        return pltpu.make_async_remote_copy(src_ref=two, dst_ref=two, send_sem=sends.at[s], recv_sem=ssem.at[s],
                                            device_id={"sp": sib}, device_id_type=MESH)

    def finish(s, _):
        o = mix_s[s, :HEAD, :] * (1 / mix_s[s, HEAD : HEAD + 1, :])
        for i in range(2):
            seen[c, 2 * s + i] = o[:, i * T : (i + 1) * T].T.astype(BF16)
        share(s).start()
        return 0

    lax.fori_loop(0, NS, finish, 0)

    def lhs(k):
        return jnp.concatenate([seen[k, i] for i in range(NH)], axis=1)

    def share_of(k, j):
        return _dot(lhs(k), pool[j, pl.ds(pl.multiple_of(k * NH * HEAD, NH * HEAD), NH * HEAD), :], 1, 0)

    def out_own(j, _):
        load_wo(j).wait()
        accy[j] = share_of(c, j)
        return 0

    lax.fori_loop(0, NC, out_own, 0)
    for s in range(NS):
        share(s).wait()
    for j in range(NC):
        xr_cp[j].wait()
        wait_for(xr.at[j, theirs, :], xrsem.at[j])

    def out_there(j, k):
        return pltpu.make_async_remote_copy(src_ref=ybuf.at[j, theirs, :], dst_ref=o_h.at[:, cols(k, j)], send_sem=sends.at[NS + j],
                                            recv_sem=ysem.at[j], device_id={"sp": sib}, device_id_type=MESH)

    def out_rest(j, _):
        y = accy[j] + share_of(oc, j)
        ybuf[j] = (xr[j].astype(F32) + y).astype(BF16)
        out_there(j, c).start()
        o_h[:, cols(c, j)] = ybuf[j, mine, :]
        return 0

    lax.fori_loop(0, NC, out_rest, 0)
    for ref, i, cond in sent:
        if cond is None:
            wait_for(ref, send.at[i])
        else:
            pl.when(cond)(functools.partial(wait_for, ref, send.at[i]))
    for j in range(NC):
        out_there(j, oc).wait()


def solution(mesh):
    n = mesh.shape["sp"]
    chips = n // 2
    S = math.isqrt(chips)

    def tables(own):
        half = HEAD // 2
        rate = (np.float32(THETA) ** (-np.arange(half, dtype=np.float32) / np.float32(half))).astype(np.float64)

        def pair(place):
            angle = place[:, None] * rate
            cos, sin = np.cos(angle), np.sin(angle)
            return np.concatenate([cos, cos], 1), np.concatenate([-sin, sin], 1)

        ta = np.stack(pair(np.arange(2 * own, dtype=np.float64)))
        tb = np.stack(pair(np.arange(chips, dtype=np.float64) * 2 * own), 1)
        return ta.astype(np.float32), tb.astype(np.float32)

    def step(x, gain, wq, wk, wv, wo):
        own, D = x.shape
        NH = wq.shape[1] // HEAD // 2
        KV = wk.shape[1] // HEAD // 2
        CW = wk.shape[1]
        NC = NH * HEAD // CW
        T, W, NS = 2 * own, 4 * own, NH // 2
        ta, tb = tables(own)
        any_ = pl.BlockSpec(memory_space=pl.ANY)
        dma = pltpu.SemaphoreType.DMA
        return pl.pallas_call(
            functools.partial(_kernel, (S, own, D, CW, NH)),
            out_shape=pltpu.VMEM(x.shape, x.dtype),
            in_specs=[any_] * 8,
            out_specs=pl.BlockSpec(memory_space=pltpu.VMEM),
            scratch_shapes=[
                pltpu.VMEM((2 + NC, D, CW), BF16),
                pltpu.VMEM((own, D), BF16),
                pltpu.VMEM((D,), BF16),
                pltpu.VMEM((T, D), BF16),
                pltpu.VMEM((NC, T, CW), BF16),
                pltpu.VMEM((2, T, HEAD), F32),
                pltpu.VMEM((chips, 2, HEAD), F32),
                pltpu.VMEM((2, T, HEAD), F32),
                pltpu.VMEM((2 * KV, own, HEAD), BF16),
                pltpu.VMEM((2 * KV, HEAD, own), BF16),
                pltpu.VMEM((S, KV, S * T, HEAD), BF16),
                pltpu.VMEM((S, KV, HEAD, S * T), BF16),
                pltpu.VMEM((NH * T, HEAD), BF16),
                pltpu.VMEM((NS, HEAD + 8, W), F32),
                pltpu.VMEM((NS, 1, W), F32),
                pltpu.VMEM((2, NH, T, HEAD), BF16),
                pltpu.VMEM((NC, T, CW), F32),
                pltpu.VMEM((NC, T, CW), BF16),
                pltpu.VMEM((T, W), jnp.int32),
                pltpu.VMEM((4 * T, W), F32),
                pltpu.VMEM((4 * T, W), F32),
                pltpu.VMEM((4, W), F32),
                pltpu.VMEM((4, W), F32),
                dma((2 + 2 * NC,)),
                dma((4 + 2 * NC,)),
                dma((S, S)),
                dma((S, S)),
                dma((2,)),
                dma,
                dma((NC,)),
                dma((NS,)),
                dma((NC,)),
                dma((NS + NC,)),
                dma((80,)),
            ],
            compiler_params=pltpu.CompilerParams(
                collective_id=0, has_side_effects=True, vmem_limit_bytes=VMEM,
                ),
        )(x, gain, wq, wk, wv, wo, ta, tb)

    tokens, whole = P(("dp", "sp"), None), P(None, None)
    return jax.shard_map(
        step,
        mesh=mesh,
        in_specs=(tokens, P(None), whole, whole, whole, whole),
        out_specs=tokens,
        check_vma=False,
    )
```

```python
import functools
import math

import jax
import jax.numpy as jnp
import numpy as np
from jax import lax
from jax.experimental import pallas as pl
from jax.experimental.pallas import tpu as pltpu
from jax.sharding import PartitionSpec as P

HEAD = 128
THETA = 10000
HIDDEN = -2e30
NONE = -1e30
BIG = 1e30
LOG2E = 1.4426950408889634
VMEM = 60 * 2**20
MESH = pl.DeviceIdType.MESH
F32, BF16 = jnp.float32, jnp.bfloat16


def _dot(a, b, ca, cb):
    return lax.dot_general(a, b, (((ca,), (cb,)), ((), ())), preferred_element_type=F32)


BLOCKS = ((0, 0), (1, 0), (3, 0), (0, 1), (0, 3), (3, 3), (1, 1), (1, 3), (3, 1), (2, 0), (0, 2), (2, 1), (2, 3), (3, 2), (1, 2), (2, 2))
EVENTS = (
    (1, 3, 0), (1, 1, 0), (0, 0, 3), (0, 0, 1), (0, 2, 0), (1, 1, 3), (0, 3, 3), (0, 3, 1), (1, 3, 3), (1, 1, 1), (0, 1, 3), (0, 1, 1), (1, 3, 1),
    (1, 2, 0), (1, 0, 2), (0, 2, 1), (1, 2, 3), (0, 0, 2), (1, 2, 1), (0, 2, 3), (0, 3, 2), (1, 1, 2), (1, 3, 2), (0, 1, 2), (0, 2, 2), (1, 2, 2),
)
TIMES = (140, 140, 147, 147, 167, 169, 175, 175, 196, 197, 203, 203, 210, 224, 231, 231, 239, 246, 254, 260, 274, 279, 281, 288, 302, 315)
START, STEP = 145, 16


def _kernel(cfg, x_h, g_h, wq_h, wk_h, wv_h, wo_h, ta_h, tb_h, o_h,
            pool, xs, gs, a_s, xr, ta, tb, cs, stage_k, stage_v, kb, vb, q_s, mix_s, top_s, seen, accy, ybuf,
            gap, sc0, sc1, mx0, mx1,
            wsem, lsem, ksem, vsem, ownsem, asem, xrsem, ssem, ysem, sends, send):
    sc, mx = (sc0, sc1), (mx0, mx1)
    S, own, D, CW, NH = cfg
    T = 2 * own
    KV = 2
    NC = NH * HEAD // CW
    HC = CW // HEAD
    W = 2 * T
    NS = NH // 2
    e = HEAD**-0.5 * LOG2E

    me = lax.axis_index("sp")
    c = lax.rem(me, 2)
    chip = lax.div(me, 2)
    X, Y = lax.div(chip, S), lax.rem(chip, S)
    oc = 1 - c
    sg = 1 - 2 * c
    sib = chip * 2 + oc

    @functools.cache
    def at(a, b):
        return lax.rem(X + sg * a + S, S), lax.rem(Y + sg * b + S, S)

    def dev(xy, k):
        return (xy[0] * S + xy[1]) * 2 + k

    for a_ in range(4):
        for b_ in range(4):
            at(a_, b_)
    NX, PX, NY, PY = at(1, 0), at(3, 0), at(0, 1), at(0, 3)

    def local(src, dst, sem):
        cp = pltpu.make_async_copy(src, dst, sem)
        cp.start()
        return cp

    x_cp = local(x_h, xs, lsem.at[0])
    g_cp = local(g_h, gs, lsem.at[1])
    wk_cp = local(wk_h, pool.at[0], wsem.at[0])
    wv_cp = local(wv_h, pool.at[1], wsem.at[1])
    ta_cp = local(ta_h, ta, lsem.at[2])
    tb_cp = local(tb_h, tb, lsem.at[3])

    barrier = pltpu.get_barrier_semaphore()
    greet = [sib] + [dev(n, k) for n in (NX, PX, NY, PY) for k in range(2)]
    for d in greet:
        pl.semaphore_signal(barrier, inc=1, device_id={"sp": d}, device_id_type=MESH)

    def needs(kind, s, d, sg=sg):
        (sx, sy), (dx, dy) = s, d
        ahead = lambda v: lax.rem(v + sg + S, S)
        if kind == 0:
            along = (sx < dx) | ((ahead(sx) == dx) & (sx < ahead(dx)))
            across = (sx < dx) | ((sx == dx) & ((sy < dy) | ((ahead(sy) == dy) & (sy < ahead(dy)))))
            return jnp.where(sy == dy, along, across)
        along = (sx < S - 1) | (sy < dy) | ((ahead(sy) == dy) & (sy < ahead(dy)))
        across = (sx < dx) | ((ahead(sx) == dx) & (sx < ahead(dx)))
        return jnp.where(sx == dx, along, across)

    me_xy = (X, Y)
    routes = {}
    for kind in range(2):
        one, two = ((NX, PX), (NY, PY)) if kind == 0 else ((NY, PY), (NX, PX))
        for a in range(4):
            for b in range(4):
                xy = at(*((a, b) if kind == 0 else (b, a)))
                to = ([one[0]] if a == 3 else []) + [two[0], two[1]] if b == 0 else [two[0]] if b == 3 else []
                if (a, b) != (0, 0):
                    routes[kind, a, b] = xy, needs(kind, xy, me_xy), [(n, needs(kind, xy, n)) for n in to]

    U = 2
    n = 4
    per = NS // U
    last = len(EVENTS) - 1
    rank, code = [], []
    nv = 0
    for a, b in BLOCKS:
        x, y = at(a, b)
        vis = x * S + y <= chip
        need = max([i for i, (_, p, q) in enumerate(EVENTS) if (p, q) == (a, b)], default=0)
        rank.append(jnp.where(vis, nv, -1))
        code.append((1 << 16) + (need << 8) + (x << 4) + y)
        nv = nv + vis.astype(jnp.int32)
        if len(rank) == n + 1:
            nv = jnp.maximum(nv, n)
    groups = jnp.maximum(jnp.where(nv == len(BLOCKS), lax.div(nv, n), lax.div(nv - 1, n)), 1)
    singles = jnp.maximum(nv - n * groups, 0)

    slots_ = []
    for k in range(len(BLOCKS)):
        got = functools.reduce(jnp.add, [jnp.where(r == k, v, 0) for r, v in zip(rank, code)])
        slots_.append(jnp.where(got > 0, got, code[0] - (1 << 16)))

    gap[...] = lax.rem(lax.broadcasted_iota(jnp.int32, (T, W), 1), T) - lax.broadcasted_iota(jnp.int32, (T, W), 0)
    top_s[...] = jnp.full(top_s.shape, NONE, F32)
    mix_s[...] = jnp.zeros(mix_s.shape, F32)

    sent = []

    def push(src, dst, rsem, device, like=None, cond=None):
        cp = pltpu.make_async_remote_copy(src_ref=src, dst_ref=dst, send_sem=send.at[len(sent)], recv_sem=rsem,
                                          device_id={"sp": device}, device_id_type=MESH)
        if cond is None:
            cp.start()
        else:
            pl.when(cond)(cp.start)
        sent.append((src if like is None else like, len(sent), cond))

    def wait_for(ref, sem):
        pltpu.make_async_copy(ref, ref, sem).wait()

    def cols(k, j):
        return pl.ds(pl.multiple_of(k * (NH * HEAD) + j * CW, CW), CW)

    mine = pl.ds(pl.multiple_of(c * own, own), own)
    theirs = pl.ds(pl.multiple_of(oc * own, own), own)

    def load_wq(j):
        return pltpu.make_async_copy(wq_h.at[:, cols(c, j)], pool.at[2 + j], wsem.at[2 + j])

    def load_wo(j):
        return pltpu.make_async_copy(wo_h.at[:, cols(c, j)], pool.at[j], wsem.at[2 + NC + j])

    x_cp.wait()
    g_cp.wait()
    RG = 32

    def norm(r, _):
        rows = pl.ds(pl.multiple_of(r * RG, RG), RG)
        wide = xs[rows, :].astype(F32)
        scale = lax.rsqrt(jnp.sum(wide * wide, axis=-1, keepdims=True) * (1 / D) + 1e-6)
        a_s[pl.ds(pl.multiple_of(c * own + r * RG, RG), RG), :] = (wide * scale * gs[...].reshape(1, D).astype(F32)).astype(BF16)
        return 0

    lax.fori_loop(0, own // RG, norm, 0)
    for j in range(NC // 2):
        load_wq(j).start()
    pl.semaphore_wait(barrier, len(greet))
    push(a_s.at[mine, :], a_s.at[mine, :], asem, sib)

    ta_cp.wait()
    tb_cp.wait()
    cb, sb = tb[chip, 0:1, :], tb[chip, 1:2, :]
    ca, sa = ta[0], ta[1]
    cs[0] = ca * cb - sa * sb
    cs[1] = sa * cb + ca * sb

    def turned(t, cos, sin):
        t = t.astype(BF16).astype(F32)
        return (t * cos + pltpu.roll(t, HEAD // 2, 1) * sin).astype(BF16)

    def block(ref, xy, kind):
        span = pl.ds(pl.multiple_of(xy[1] * T, T), T)
        return ref.at[xy[0], :, span, :] if kind == 0 else ref.at[xy[0], :, :, span]

    def part(ref, xy, kind, k):
        span = pl.ds(pl.multiple_of(xy[1] * T + k * own, own), own)
        return ref.at[xy[0], :, span, :] if kind == 0 else ref.at[xy[0], :, :, span]

    sems = (ksem, vsem)
    bufs = (kb, vb)
    stages = (stage_k, stage_v)
    whole = (block(kb, me_xy, 0), block(vb, me_xy, 1))

    def own_out(kind, n):
        for k in range(2):
            push(stages[kind].at[pl.ds(KV * k, KV)], part(bufs[kind], me_xy, kind, c), sems[kind].at[X, Y], dev(n, k), cond=needs(kind, me_xy, n, 1 - 2 * k))

    wk_cp.wait()
    for j in range(NC // 2, NC):
        load_wq(j).start()
    k_all = _dot(a_s[mine, :], pool[0], 1, 0)
    cos, sin = cs[0, mine, :], cs[1, mine, :]
    for h in range(2 * KV):
        stage_k[h] = turned(k_all[:, h * HEAD : (h + 1) * HEAD], cos, sin)
    span = pl.ds(pl.multiple_of(Y * T + c * own, own), own)
    for h in range(KV):
        kb[X, h, span, :] = stage_k[KV * c + h]
    own_out(0, NX)
    own_out(0, PX)
    push(stage_k.at[pl.ds(KV * oc, KV)], part(kb, me_xy, 0, c), ownsem.at[0], sib)

    wv_cp.wait()
    v_all = _dot(a_s[mine, :], pool[1], 1, 0).astype(BF16)
    for h in range(2 * KV):
        stage_v[h] = v_all[:, h * HEAD : (h + 1) * HEAD].T
    for h in range(KV):
        vb[X, h, :, span] = stage_v[KV * c + h]
    own_out(1, NY)
    own_out(1, PY)
    own_out(0, NY)
    own_out(0, PY)
    own_out(1, NX)
    own_out(1, PX)
    push(stage_v.at[pl.ds(KV * oc, KV)], part(vb, me_xy, 1, c), ownsem.at[1], sib)

    xr_cp = [local(x_h.at[:, cols(c, j)], xr.at[j, mine, :], lsem.at[4 + j]) for j in range(NC)]
    for j in range(NC):
        push(x_h.at[:, cols(oc, j)], xr.at[j, mine, :], xrsem.at[j], sib)

    def forward(kind, a, b):
        xy, here, to = routes[kind, a, b]
        ref = block(bufs[kind], xy, kind)
        sem = sems[kind].at[xy[0], xy[1]]

        @pl.when(here)
        def _():
            wait_for(ref, sem)

        for n, cond in to:
            push(ref, ref, sem, dev(n, c), like=whole[kind], cond=cond)

    wait_for(a_s.at[theirs, :], asem)

    def queries(j, _):
        load_wq(j).wait()
        q = _dot(a_s[...], pool[2 + j], 1, 0)
        for i in range(HC):
            rows = pl.ds(pl.multiple_of((j * HC + i) * T, T), T)
            q_s[rows, :] = turned(q[:, i * HEAD : (i + 1) * HEAD], cs[0], cs[1])
        load_wo(j).start()

        @pl.when(j == NC - 2)
        def _():
            forward(0, 3, 0)
            forward(0, 1, 0)

        return 0

    lax.fori_loop(0, NC, queries, 0)
    forward(1, 3, 0)
    forward(1, 1, 0)
    wait_for(part(kb, me_xy, 0, oc), ownsem.at[0])
    wait_for(part(vb, me_xy, 1, oc), ownsem.at[1])
    def pick(k, values):
        out = values[0]
        for i in range(1, len(values)):
            out = jnp.where(k == i, values[i], out)
        return out

    def score(s, slots):
        h = lax.div(s * KV, NS)
        q = q_s[pl.ds(pl.multiple_of(s * W, W), W), :]
        k = [kb[x, h, pl.ds(pl.multiple_of(y * T, T), T), :] for _, x, y, _ in slots]
        return _dot(jnp.concatenate(k, axis=0), q, 1, 1)

    def take(s, slots, parts, tops):
        h = lax.div(s * KV, NS)
        old = top_s[s]
        tops = [jnp.where(slot[3], top, NONE) for slot, top in zip(slots, tops)]
        top = functools.reduce(jnp.maximum, tops, old)
        top_s[s] = top
        p = [jnp.exp2((parts(i) - jnp.where(slot[3], top, BIG)) * e).astype(BF16) for i, slot in enumerate(slots)]
        keep = jnp.exp2((old - top) * e)
        v = [vb[x, h, :, pl.ds(pl.multiple_of(y * T, T), T)] for _, x, y, _ in slots]
        v = jnp.concatenate([jnp.concatenate(v, axis=1), jnp.ones((8, len(slots) * T), BF16)], axis=0)
        mix_s[s] = mix_s[s] * keep + _dot(v, jnp.concatenate(p, axis=0), 1, 0)

    def split(t, m):
        return [t[i * T : (i + 1) * T] for i in range(m)]

    def put(s, b, slots, cut):
        t = split(score(s, slots), n)
        if cut:
            t[0] = jnp.where(gap[...] >= 0, t[0], HIDDEN)
        for i in range(n):
            sc[b][i * T : (i + 1) * T, :] = t[i]
        mx[b][...] = jnp.concatenate([v.max(axis=0, keepdims=True) for v in t], axis=0)

    def fin(s, b, slots):
        take(s, slots, lambda i: sc[b][i * T : (i + 1) * T, :], [mx[b][i : i + 1, :] for i in range(n)])

    def pair(i, slots, cut):
        put(2 * i + 1, 1, slots, cut)
        fin(2 * i, 0, slots)
        put(jnp.minimum(2 * i + 2, NS - 1), 0, slots, cut)
        fin(2 * i + 1, 1, slots)

    def single(slots):
        ts = [score(s, slots) for s in range(NS)]
        for s, t in enumerate(ts):
            take(s, slots, lambda i: t, [t.max(axis=0, keepdims=True)])

    def step(t, carry):
        done, clock = carry
        g = lax.div(t, per)
        grouped = t < per * groups
        k = jnp.where(grouped, n * g, n * groups + t - per * groups)
        got = [pick(g, slots_[j::n]) for j in range(n)]
        got[0] = jnp.where(grouped, got[0], pick(k, slots_))
        slots = [((v >> 8) & 255, (v >> 4) & 15, v & 15, v >= 1 << 16) for v in got]
        target = functools.reduce(jnp.maximum, [jnp.where(slots[j][3] & (grouped | (j == 0)), slots[j][0], 0) for j in range(n)])
        for i, time in enumerate(TIMES):
            clock = jnp.maximum(clock, jnp.where(target == i, time, 0))
        come = functools.reduce(jnp.add, [jnp.where(clock >= time, 1, 0) for time in TIMES])
        target = jnp.maximum(target, come - 1)
        target = jnp.where(t == per * groups + singles, last, target)

        @pl.when(target > done)
        def _():
            for i, (kind, a, b) in enumerate(EVENTS):

                @pl.when((i > done) & (i <= target))
                def _():
                    forward(kind, *((a, b) if kind == 0 else (b, a)))

        i = lax.rem(t, per)

        for cut in (True, False):
            these = (g == 0) if cut else (grouped & (g > 0))

            @pl.when(these & (i == 0))
            def _():
                put(0, 0, slots, cut)

            @pl.when(these)
            def _():
                pair(i, slots, cut)

        @pl.when((t >= per * groups) & (t < per * groups + singles))
        def _():
            single(slots[:1])

        return jnp.maximum(done, target), clock + STEP

    lax.fori_loop(0, per * groups + singles + 1, step, (-1, START))

    def share(s):
        two = seen.at[c, pl.ds(2 * s, 2)]
        return pltpu.make_async_remote_copy(src_ref=two, dst_ref=two, send_sem=sends.at[s], recv_sem=ssem.at[s],
                                            device_id={"sp": sib}, device_id_type=MESH)

    def finish(s, _):
        o = (mix_s[s, :HEAD, :] * (1 / mix_s[s, HEAD : HEAD + 1, :])).astype(BF16)
        for i in range(2):
            seen[c, 2 * s + i] = o[:, i * T : (i + 1) * T].T
        share(s).start()
        return 0

    lax.fori_loop(0, NS, finish, 0, unroll=4)

    def lhs(k):
        return jnp.concatenate([seen[k, i] for i in range(NH)], axis=1)

    def share_of(k, j):
        return _dot(lhs(k), pool[j, pl.ds(pl.multiple_of(k * NH * HEAD, NH * HEAD), NH * HEAD), :], 1, 0)

    def out_own(j, _):
        accy[j] = share_of(c, j)
        return 0

    for j in range(NC):
        load_wo(j).wait()
    lax.fori_loop(0, NC, out_own, 0, unroll=4)
    for s in range(NS):
        share(s).wait()
    for j in range(NC):
        xr_cp[j].wait()
        wait_for(xr.at[j, theirs, :], xrsem.at[j])

    def out_there(j, k):
        return pltpu.make_async_remote_copy(src_ref=ybuf.at[j, theirs, :], dst_ref=o_h.at[:, cols(k, j)], send_sem=sends.at[NS + j],
                                            recv_sem=ysem.at[j], device_id={"sp": sib}, device_id_type=MESH)

    def out_rest(j, _):
        y = accy[j] + share_of(oc, j)
        ybuf[j] = (xr[j].astype(F32) + y).astype(BF16)
        out_there(j, c).start()
        o_h[:, cols(c, j)] = ybuf[j, mine, :]
        return 0

    lax.fori_loop(0, NC, out_rest, 0, unroll=4)
    for ref, i, cond in sent:
        if cond is None:
            wait_for(ref, send.at[i])
        else:
            pl.when(cond)(functools.partial(wait_for, ref, send.at[i]))
    for j in range(NC):
        out_there(j, oc).wait()


def solution(mesh):
    n = mesh.shape["sp"]
    chips = n // 2
    S = math.isqrt(chips)

    def tables(own):
        half = HEAD // 2
        rate = (np.float32(THETA) ** (-np.arange(half, dtype=np.float32) / np.float32(half))).astype(np.float64)

        def pair(place):
            angle = place[:, None] * rate
            cos, sin = np.cos(angle), np.sin(angle)
            return np.concatenate([cos, cos], 1), np.concatenate([-sin, sin], 1)

        ta = np.stack(pair(np.arange(2 * own, dtype=np.float64)))
        tb = np.stack(pair(np.arange(chips, dtype=np.float64) * 2 * own), 1)
        return ta.astype(np.float32), tb.astype(np.float32)

    def step(x, gain, wq, wk, wv, wo):
        own, D = x.shape
        NH = wq.shape[1] // HEAD // 2
        KV = wk.shape[1] // HEAD // 2
        CW = wk.shape[1]
        NC = NH * HEAD // CW
        T, W, NS = 2 * own, 4 * own, NH // 2
        ta, tb = tables(own)
        any_ = pl.BlockSpec(memory_space=pl.ANY)
        dma = pltpu.SemaphoreType.DMA
        return pl.pallas_call(
            functools.partial(_kernel, (S, own, D, CW, NH)),
            out_shape=pltpu.VMEM(x.shape, x.dtype),
            in_specs=[any_] * 8,
            out_specs=pl.BlockSpec(memory_space=pltpu.VMEM),
            scratch_shapes=[
                pltpu.VMEM((2 + NC, D, CW), BF16),
                pltpu.VMEM((own, D), BF16),
                pltpu.VMEM((D,), BF16),
                pltpu.VMEM((T, D), BF16),
                pltpu.VMEM((NC, T, CW), BF16),
                pltpu.VMEM((2, T, HEAD), F32),
                pltpu.VMEM((chips, 2, HEAD), F32),
                pltpu.VMEM((2, T, HEAD), F32),
                pltpu.VMEM((2 * KV, own, HEAD), BF16),
                pltpu.VMEM((2 * KV, HEAD, own), BF16),
                pltpu.VMEM((S, KV, S * T, HEAD), BF16),
                pltpu.VMEM((S, KV, HEAD, S * T), BF16),
                pltpu.VMEM((NH * T, HEAD), BF16),
                pltpu.VMEM((NS, HEAD + 8, W), F32),
                pltpu.VMEM((NS, 1, W), F32),
                pltpu.VMEM((2, NH, T, HEAD), BF16),
                pltpu.VMEM((NC, T, CW), F32),
                pltpu.VMEM((NC, T, CW), BF16),
                pltpu.VMEM((T, W), jnp.int32),
                pltpu.VMEM((4 * T, W), F32),
                pltpu.VMEM((4 * T, W), F32),
                pltpu.VMEM((4, W), F32),
                pltpu.VMEM((4, W), F32),
                dma((2 + 2 * NC,)),
                dma((4 + 2 * NC,)),
                dma((S, S)),
                dma((S, S)),
                dma((2,)),
                dma,
                dma((NC,)),
                dma((NS,)),
                dma((NC,)),
                dma((NS + NC,)),
                dma((80,)),
            ],
            compiler_params=pltpu.CompilerParams(
                collective_id=0, has_side_effects=True, vmem_limit_bytes=VMEM,
                ),
        )(x, gain, wq, wk, wv, wo, ta, tb)

    tokens, whole = P(("dp", "sp"), None), P(None, None)
    return jax.shard_map(
        step,
        mesh=mesh,
        in_specs=(tokens, P(None), whole, whole, whole, whole),
        out_specs=tokens,
        check_vma=False,
    )
```

```python
import functools
import math

import jax
import jax.numpy as jnp
import numpy as np
from jax import lax
from jax.experimental import pallas as pl
from jax.experimental.pallas import tpu as pltpu
from jax.sharding import PartitionSpec as P

HEAD = 128
THETA = 10000
HIDDEN = -2e30
NONE = -1e30
BIG = 1e30
LOG2E = 1.4426950408889634
VMEM = 60 * 2**20
MESH = pl.DeviceIdType.MESH
F32, BF16 = jnp.float32, jnp.bfloat16


def _dot(a, b, ca, cb):
    return lax.dot_general(a, b, (((ca,), (cb,)), ((), ())), preferred_element_type=F32)


BLOCKS = ((0, 0), (1, 0), (3, 0), (0, 1), (0, 3), (3, 3), (1, 1), (1, 3), (3, 1), (2, 0), (0, 2), (2, 1), (2, 3), (3, 2), (1, 2), (2, 2))
EVENTS = (
    (1, 3, 0), (1, 1, 0), (0, 0, 3), (0, 0, 1), (0, 2, 0), (1, 1, 3), (0, 3, 3), (0, 3, 1), (1, 3, 3), (1, 1, 1), (0, 1, 3), (0, 1, 1), (1, 3, 1),
    (1, 2, 0), (1, 0, 2), (0, 2, 1), (1, 2, 3), (0, 0, 2), (1, 2, 1), (0, 2, 3), (0, 3, 2), (1, 1, 2), (1, 3, 2), (0, 1, 2), (0, 2, 2), (1, 2, 2),
)
TIMES = (140, 140, 147, 147, 167, 169, 175, 175, 196, 197, 203, 203, 210, 224, 231, 231, 239, 246, 254, 260, 274, 279, 281, 288, 302, 315)
START, STEP = 145, 16


def _kernel(cfg, x_h, g_h, wq_h, wk_h, wv_h, wo_h, ta_h, tb_h, o_h,
            pool, xs, gs, a_s, xr, ta, tb, cs, stage_k, stage_v, kb, vb, q_s, mix_s, top_s, seen, accy, ybuf,
            gap, sc0, sc1, mx0, mx1,
            wsem, lsem, ksem, vsem, ownsem, asem, xrsem, ssem, ysem, sends, send):
    sc, mx = (sc0, sc1), (mx0, mx1)
    S, own, D, CW, NH = cfg
    T = 2 * own
    KV = 2
    NC = NH * HEAD // CW
    HC = CW // HEAD
    W = 2 * T
    NS = NH // 2
    e = HEAD**-0.5 * LOG2E

    me = lax.axis_index("sp")
    c = lax.rem(me, 2)
    chip = lax.div(me, 2)
    X, Y = lax.div(chip, S), lax.rem(chip, S)
    oc = 1 - c
    sg = 1 - 2 * c
    sib = chip * 2 + oc

    @functools.cache
    def at(a, b):
        return lax.rem(X + sg * a + S, S), lax.rem(Y + sg * b + S, S)

    def dev(xy, k):
        return (xy[0] * S + xy[1]) * 2 + k

    for a_ in range(4):
        for b_ in range(4):
            at(a_, b_)
    NX, PX, NY, PY = at(1, 0), at(3, 0), at(0, 1), at(0, 3)

    def local(src, dst, sem):
        cp = pltpu.make_async_copy(src, dst, sem)
        cp.start()
        return cp

    x_cp = local(x_h, xs, lsem.at[0])
    g_cp = local(g_h, gs, lsem.at[1])
    wk_cp = local(wk_h, pool.at[0], wsem.at[0])
    wv_cp = local(wv_h, pool.at[1], wsem.at[1])
    ta_cp = local(ta_h, ta, lsem.at[2])
    tb_cp = local(tb_h, tb, lsem.at[3])

    barrier = pltpu.get_barrier_semaphore()
    greet = [sib] + [dev(n, k) for n in (NX, PX, NY, PY) for k in range(2)]
    for d in greet:
        pl.semaphore_signal(barrier, inc=1, device_id={"sp": d}, device_id_type=MESH)

    def needs(kind, s, d, sg=sg):
        (sx, sy), (dx, dy) = s, d
        ahead = lambda v: lax.rem(v + sg + S, S)
        if kind == 0:
            along = (sx < dx) | ((ahead(sx) == dx) & (sx < ahead(dx)))
            across = (sx < dx) | ((sx == dx) & ((sy < dy) | ((ahead(sy) == dy) & (sy < ahead(dy)))))
            return jnp.where(sy == dy, along, across)
        along = (sx < S - 1) | (sy < dy) | ((ahead(sy) == dy) & (sy < ahead(dy)))
        across = (sx < dx) | ((ahead(sx) == dx) & (sx < ahead(dx)))
        return jnp.where(sx == dx, along, across)

    me_xy = (X, Y)
    routes = {}
    for kind in range(2):
        one, two = ((NX, PX), (NY, PY)) if kind == 0 else ((NY, PY), (NX, PX))
        for a in range(4):
            for b in range(4):
                xy = at(*((a, b) if kind == 0 else (b, a)))
                to = ([one[0]] if a == 3 else []) + [two[0], two[1]] if b == 0 else [two[0]] if b == 3 else []
                if (a, b) != (0, 0):
                    routes[kind, a, b] = xy, needs(kind, xy, me_xy), [(n, needs(kind, xy, n)) for n in to]

    U = 2
    n = 4
    per = NS // U
    last = len(EVENTS) - 1
    rank, code = [], []
    nv = 0
    for a, b in BLOCKS:
        x, y = at(a, b)
        vis = x * S + y <= chip
        need = max([i for i, (_, p, q) in enumerate(EVENTS) if (p, q) == (a, b)], default=0)
        rank.append(jnp.where(vis, nv, -1))
        code.append((1 << 16) + (need << 8) + (x << 4) + y)
        nv = nv + vis.astype(jnp.int32)
        if len(rank) == n + 1:
            nv = jnp.maximum(nv, n)
    groups = jnp.maximum(jnp.where(nv == len(BLOCKS), lax.div(nv, n), lax.div(nv - 1, n)), 1)
    singles = jnp.maximum(nv - n * groups, 0)

    slots_ = []
    for k in range(len(BLOCKS)):
        got = functools.reduce(jnp.add, [jnp.where(r == k, v, 0) for r, v in zip(rank, code)])
        slots_.append(jnp.where(got > 0, got, code[0] - (1 << 16)))

    gap[...] = lax.rem(lax.broadcasted_iota(jnp.int32, (T, W), 1), T) - lax.broadcasted_iota(jnp.int32, (T, W), 0)
    top_s[...] = jnp.full(top_s.shape, NONE, F32)
    mix_s[...] = jnp.zeros(mix_s.shape, F32)

    sent = []

    def push(src, dst, rsem, device, like=None, cond=None):
        cp = pltpu.make_async_remote_copy(src_ref=src, dst_ref=dst, send_sem=send.at[len(sent)], recv_sem=rsem,
                                          device_id={"sp": device}, device_id_type=MESH)
        if cond is None:
            cp.start()
        else:
            pl.when(cond)(cp.start)
        sent.append((src if like is None else like, len(sent), cond))

    def wait_for(ref, sem):
        pltpu.make_async_copy(ref, ref, sem).wait()

    def cols(k, j):
        return pl.ds(pl.multiple_of(k * (NH * HEAD) + j * CW, CW), CW)

    mine = pl.ds(pl.multiple_of(c * own, own), own)
    theirs = pl.ds(pl.multiple_of(oc * own, own), own)

    def load_wq(j):
        return pltpu.make_async_copy(wq_h.at[:, cols(c, j)], pool.at[2 + j], wsem.at[2 + j])

    def load_wo(j):
        return pltpu.make_async_copy(wo_h.at[:, cols(c, j)], pool.at[j], wsem.at[2 + NC + j])

    x_cp.wait()
    g_cp.wait()
    RG = 32

    def norm(r, _):
        rows = pl.ds(pl.multiple_of(r * RG, RG), RG)
        wide = xs[rows, :].astype(F32)
        scale = lax.rsqrt(jnp.sum(wide * wide, axis=-1, keepdims=True) * (1 / D) + 1e-6)
        a_s[pl.ds(pl.multiple_of(c * own + r * RG, RG), RG), :] = (wide * scale * gs[...].reshape(1, D).astype(F32)).astype(BF16)
        return 0

    lax.fori_loop(0, own // RG, norm, 0, unroll=own // RG)
    for j in range(NC // 2):
        load_wq(j).start()
    pl.semaphore_wait(barrier, len(greet))
    push(a_s.at[mine, :], a_s.at[mine, :], asem, sib)

    ta_cp.wait()
    tb_cp.wait()
    cb, sb = tb[chip, 0:1, :], tb[chip, 1:2, :]
    ca, sa = ta[0], ta[1]
    cs[0] = ca * cb - sa * sb
    cs[1] = sa * cb + ca * sb

    def turned(t, cos, sin):
        t = t.astype(BF16).astype(F32)
        return (t * cos + pltpu.roll(t, HEAD // 2, 1) * sin).astype(BF16)

    def block(ref, xy, kind):
        span = pl.ds(pl.multiple_of(xy[1] * T, T), T)
        return ref.at[xy[0], :, span, :] if kind == 0 else ref.at[xy[0], :, :, span]

    def part(ref, xy, kind, k):
        span = pl.ds(pl.multiple_of(xy[1] * T + k * own, own), own)
        return ref.at[xy[0], :, span, :] if kind == 0 else ref.at[xy[0], :, :, span]

    sems = (ksem, vsem)
    bufs = (kb, vb)
    stages = (stage_k, stage_v)
    whole = (block(kb, me_xy, 0), block(vb, me_xy, 1))

    def own_out(kind, n):
        for k in range(2):
            push(stages[kind].at[pl.ds(KV * k, KV)], part(bufs[kind], me_xy, kind, c), sems[kind].at[X, Y], dev(n, k), cond=needs(kind, me_xy, n, 1 - 2 * k))

    wk_cp.wait()
    for j in range(NC // 2, NC):
        load_wq(j).start()
    k_all = _dot(a_s[mine, :], pool[0], 1, 0)
    cos, sin = cs[0, mine, :], cs[1, mine, :]
    for h in range(2 * KV):
        stage_k[h] = turned(k_all[:, h * HEAD : (h + 1) * HEAD], cos, sin)
    span = pl.ds(pl.multiple_of(Y * T + c * own, own), own)
    for h in range(KV):
        kb[X, h, span, :] = stage_k[KV * c + h]
    own_out(0, NX)
    own_out(0, PX)
    push(stage_k.at[pl.ds(KV * oc, KV)], part(kb, me_xy, 0, c), ownsem.at[0], sib)

    wv_cp.wait()
    v_all = _dot(a_s[mine, :], pool[1], 1, 0).astype(BF16)
    for h in range(2 * KV):
        stage_v[h] = v_all[:, h * HEAD : (h + 1) * HEAD].T
    for h in range(KV):
        vb[X, h, :, span] = stage_v[KV * c + h]
    own_out(1, NY)
    own_out(1, PY)
    own_out(0, NY)
    own_out(0, PY)
    own_out(1, NX)
    own_out(1, PX)
    push(stage_v.at[pl.ds(KV * oc, KV)], part(vb, me_xy, 1, c), ownsem.at[1], sib)

    xr_cp = [local(x_h.at[:, cols(c, j)], xr.at[j, mine, :], lsem.at[4 + j]) for j in range(NC)]
    for j in range(NC):
        push(x_h.at[:, cols(oc, j)], xr.at[j, mine, :], xrsem.at[j], sib)

    def forward(kind, a, b):
        xy, here, to = routes[kind, a, b]
        ref = block(bufs[kind], xy, kind)
        sem = sems[kind].at[xy[0], xy[1]]

        @pl.when(here)
        def _():
            wait_for(ref, sem)

        for n, cond in to:
            push(ref, ref, sem, dev(n, c), like=whole[kind], cond=cond)

    wait_for(a_s.at[theirs, :], asem)

    def queries(j, _):
        load_wq(j).wait()
        q = _dot(a_s[...], pool[2 + j], 1, 0)
        for i in range(HC):
            rows = pl.ds(pl.multiple_of((j * HC + i) * T, T), T)
            q_s[rows, :] = turned(q[:, i * HEAD : (i + 1) * HEAD], cs[0], cs[1])
        load_wo(j).start()

        @pl.when(j == NC - 2)
        def _():
            forward(0, 3, 0)
            forward(0, 1, 0)

        return 0

    lax.fori_loop(0, NC, queries, 0)
    forward(1, 3, 0)
    forward(1, 1, 0)
    wait_for(part(kb, me_xy, 0, oc), ownsem.at[0])
    wait_for(part(vb, me_xy, 1, oc), ownsem.at[1])
    def pick(k, values):
        out = values[0]
        for i in range(1, len(values)):
            out = jnp.where(k == i, values[i], out)
        return out

    def score(s, slots):
        h = lax.div(s * KV, NS)
        q = q_s[pl.ds(pl.multiple_of(s * W, W), W), :]
        k = [kb[x, h, pl.ds(pl.multiple_of(y * T, T), T), :] for _, x, y, _ in slots]
        return _dot(jnp.concatenate(k, axis=0), q, 1, 1)

    def take(s, slots, parts, tops):
        h = lax.div(s * KV, NS)
        old = top_s[s]
        tops = [jnp.where(slot[3], top, NONE) for slot, top in zip(slots, tops)]
        top = functools.reduce(jnp.maximum, tops, old)
        top_s[s] = top
        p = [jnp.exp2((parts(i) - jnp.where(slot[3], top, BIG)) * e).astype(BF16) for i, slot in enumerate(slots)]
        keep = jnp.exp2((old - top) * e)
        v = [vb[x, h, :, pl.ds(pl.multiple_of(y * T, T), T)] for _, x, y, _ in slots]
        v = jnp.concatenate([jnp.concatenate(v, axis=1), jnp.ones((8, len(slots) * T), BF16)], axis=0)
        mix_s[s] = mix_s[s] * keep + _dot(v, jnp.concatenate(p, axis=0), 1, 0)

    def split(t, m):
        return [t[i * T : (i + 1) * T] for i in range(m)]

    def put(s, b, slots, cut):
        t = split(score(s, slots), n)
        if cut:
            t[0] = jnp.where(gap[...] >= 0, t[0], HIDDEN)
        for i in range(n):
            sc[b][i * T : (i + 1) * T, :] = t[i]
        mx[b][...] = jnp.concatenate([v.max(axis=0, keepdims=True) for v in t], axis=0)

    def fin(s, b, slots):
        take(s, slots, lambda i: sc[b][i * T : (i + 1) * T, :], [mx[b][i : i + 1, :] for i in range(n)])

    def pair(i, slots, cut):
        put(2 * i + 1, 1, slots, cut)
        fin(2 * i, 0, slots)
        put(jnp.minimum(2 * i + 2, NS - 1), 0, slots, cut)
        fin(2 * i + 1, 1, slots)

    def single(slots):
        ts = [score(s, slots) for s in range(NS)]
        for s, t in enumerate(ts):
            take(s, slots, lambda i: t, [t.max(axis=0, keepdims=True)])

    def step(t, carry):
        done, clock = carry
        g = lax.div(t, per)
        grouped = t < per * groups
        k = jnp.where(grouped, n * g, n * groups + t - per * groups)
        got = [pick(g, slots_[j::n]) for j in range(n)]
        got[0] = jnp.where(grouped, got[0], pick(k, slots_))
        slots = [((v >> 8) & 255, (v >> 4) & 15, v & 15, v >= 1 << 16) for v in got]
        target = functools.reduce(jnp.maximum, [jnp.where(slots[j][3] & (grouped | (j == 0)), slots[j][0], 0) for j in range(n)])
        for i, time in enumerate(TIMES):
            clock = jnp.maximum(clock, jnp.where(target == i, time, 0))
        come = functools.reduce(jnp.add, [jnp.where(clock >= time, 1, 0) for time in TIMES])
        target = jnp.maximum(target, come - 1)
        target = jnp.where(t == per * groups + singles, last, target)

        @pl.when(target > done)
        def _():
            for i, (kind, a, b) in enumerate(EVENTS):

                @pl.when((i > done) & (i <= target))
                def _():
                    forward(kind, *((a, b) if kind == 0 else (b, a)))

        i = lax.rem(t, per)

        for cut in (True, False):
            these = (g == 0) if cut else (grouped & (g > 0))

            @pl.when(these & (i == 0))
            def _():
                put(0, 0, slots, cut)

            @pl.when(these)
            def _():
                pair(i, slots, cut)

        @pl.when((t >= per * groups) & (t < per * groups + singles))
        def _():
            single(slots[:1])

        return jnp.maximum(done, target), clock + STEP

    lax.fori_loop(0, per * groups + singles + 1, step, (-1, START))

    def share(s):
        two = seen.at[c, pl.ds(2 * s, 2)]
        return pltpu.make_async_remote_copy(src_ref=two, dst_ref=two, send_sem=sends.at[s], recv_sem=ssem.at[s],
                                            device_id={"sp": sib}, device_id_type=MESH)

    def finish(s, _):
        o = (mix_s[s, :HEAD, :] * (1 / mix_s[s, HEAD : HEAD + 1, :])).astype(BF16)
        for i in range(2):
            seen[c, 2 * s + i] = o[:, i * T : (i + 1) * T].T
        share(s).start()
        return 0

    lax.fori_loop(0, NS, finish, 0, unroll=NS)

    def lhs(k):
        return jnp.concatenate([seen[k, i] for i in range(NH)], axis=1)

    def share_of(k, j):
        return _dot(lhs(k), pool[j, pl.ds(pl.multiple_of(k * NH * HEAD, NH * HEAD), NH * HEAD), :], 1, 0)

    def out_own(j, _):
        accy[j] = share_of(c, j)
        return 0

    for j in range(NC):
        load_wo(j).wait()
    lax.fori_loop(0, NC, out_own, 0, unroll=4)
    for s in range(NS):
        share(s).wait()
    for j in range(NC):
        xr_cp[j].wait()
        wait_for(xr.at[j, theirs, :], xrsem.at[j])

    def out_there(j, k):
        return pltpu.make_async_remote_copy(src_ref=ybuf.at[j, theirs, :], dst_ref=o_h.at[:, cols(k, j)], send_sem=sends.at[NS + j],
                                            recv_sem=ysem.at[j], device_id={"sp": sib}, device_id_type=MESH)

    def out_rest(j, _):
        y = accy[j] + share_of(oc, j)
        ybuf[j] = (xr[j].astype(F32) + y).astype(BF16)
        out_there(j, c).start()
        o_h[:, cols(c, j)] = ybuf[j, mine, :]
        return 0

    lax.fori_loop(0, NC, out_rest, 0, unroll=4)
    for ref, i, cond in sent:
        if cond is None:
            wait_for(ref, send.at[i])
        else:
            pl.when(cond)(functools.partial(wait_for, ref, send.at[i]))
    for j in range(NC):
        out_there(j, oc).wait()


def solution(mesh):
    n = mesh.shape["sp"]
    chips = n // 2
    S = math.isqrt(chips)

    def tables(own):
        half = HEAD // 2
        rate = (np.float32(THETA) ** (-np.arange(half, dtype=np.float32) / np.float32(half))).astype(np.float64)

        def pair(place):
            angle = place[:, None] * rate
            cos, sin = np.cos(angle), np.sin(angle)
            return np.concatenate([cos, cos], 1), np.concatenate([-sin, sin], 1)

        ta = np.stack(pair(np.arange(2 * own, dtype=np.float64)))
        tb = np.stack(pair(np.arange(chips, dtype=np.float64) * 2 * own), 1)
        return ta.astype(np.float32), tb.astype(np.float32)

    def step(x, gain, wq, wk, wv, wo):
        own, D = x.shape
        NH = wq.shape[1] // HEAD // 2
        KV = wk.shape[1] // HEAD // 2
        CW = wk.shape[1]
        NC = NH * HEAD // CW
        T, W, NS = 2 * own, 4 * own, NH // 2
        ta, tb = tables(own)
        any_ = pl.BlockSpec(memory_space=pl.ANY)
        dma = pltpu.SemaphoreType.DMA
        return pl.pallas_call(
            functools.partial(_kernel, (S, own, D, CW, NH)),
            out_shape=pltpu.VMEM(x.shape, x.dtype),
            in_specs=[any_] * 8,
            out_specs=pl.BlockSpec(memory_space=pltpu.VMEM),
            scratch_shapes=[
                pltpu.VMEM((2 + NC, D, CW), BF16),
                pltpu.VMEM((own, D), BF16),
                pltpu.VMEM((D,), BF16),
                pltpu.VMEM((T, D), BF16),
                pltpu.VMEM((NC, T, CW), BF16),
                pltpu.VMEM((2, T, HEAD), F32),
                pltpu.VMEM((chips, 2, HEAD), F32),
                pltpu.VMEM((2, T, HEAD), F32),
                pltpu.VMEM((2 * KV, own, HEAD), BF16),
                pltpu.VMEM((2 * KV, HEAD, own), BF16),
                pltpu.VMEM((S, KV, S * T, HEAD), BF16),
                pltpu.VMEM((S, KV, HEAD, S * T), BF16),
                pltpu.VMEM((NH * T, HEAD), BF16),
                pltpu.VMEM((NS, HEAD + 8, W), F32),
                pltpu.VMEM((NS, 1, W), F32),
                pltpu.VMEM((2, NH, T, HEAD), BF16),
                pltpu.VMEM((NC, T, CW), F32),
                pltpu.VMEM((NC, T, CW), BF16),
                pltpu.VMEM((T, W), jnp.int32),
                pltpu.VMEM((4 * T, W), F32),
                pltpu.VMEM((4 * T, W), F32),
                pltpu.VMEM((4, W), F32),
                pltpu.VMEM((4, W), F32),
                dma((2 + 2 * NC,)),
                dma((4 + 2 * NC,)),
                dma((S, S)),
                dma((S, S)),
                dma((2,)),
                dma,
                dma((NC,)),
                dma((NS,)),
                dma((NC,)),
                dma((NS + NC,)),
                dma((80,)),
            ],
            compiler_params=pltpu.CompilerParams(
                collective_id=0, has_side_effects=True, vmem_limit_bytes=VMEM,
                ),
        )(x, gain, wq, wk, wv, wo, ta, tb)

    tokens, whole = P(("dp", "sp"), None), P(None, None)
    return jax.shard_map(
        step,
        mesh=mesh,
        in_specs=(tokens, P(None), whole, whole, whole, whole),
        out_specs=tokens,
        check_vma=False,
    )
```
